32 devices in a mesh: dp: 1 (over z), tp: 4 (over y), fsdp: 8 (over x, core).
Axes of the slice: x: 4, y: 4, z: 1, core: 2. Of those that a mesh axis runs over, the one named last changes fastest.
The devices are a block of a 4x4x8 slice.
Arguments:
- x: bfloat16 [8, 512, 4096], P(('dp', 'fsdp'))
- w_query: bfloat16 [2, 4096, 4096], P(None, 'fsdp', 'tp')
- w_key: bfloat16 [2, 4096, 4096], P(None, 'fsdp', 'tp')
- w_value: bfloat16 [2, 4096, 4096], P(None, 'fsdp', 'tp')
- w_out: bfloat16 [2, 4096, 4096], P(None, 'tp', 'fsdp')
- w_gate: bfloat16 [2, 4096, 11008], P(None, 'fsdp', 'tp')
- w_up: bfloat16 [2, 4096, 11008], P(None, 'fsdp', 'tp')
- w_down: bfloat16 [2, 11008, 4096], P(None, 'tp', 'fsdp')
- q_norm_w: float32 [2, 4096], P(None, 'tp')
- k_norm_w: float32 [2, 4096], P(None, 'tp')
- attn_norm_w: float32 [2, 4096], P(None, 'fsdp')
- ffn_norm_w: float32 [2, 4096], P(None, 'fsdp')
Outputs:
- output 1: bfloat16 [8, 512, 4096], P(('dp', 'fsdp'))
- output 2: bfloat16 [2, 8, 512, 32, 128], P(None, ('dp', 'fsdp'), None, 'tp')
- output 3: bfloat16 [2, 8, 512, 32, 128], P(None, ('dp', 'fsdp'), None, 'tp')
All inputs are finite; a program needn't handle non-finite values.
Results may differ from the reference program's by a relative error of at most 0.02.
Values are sent between devices in bfloat16 or wider.
A program may use at most 768 MiB of HBM per device.

```python
import jax
import jax.numpy as jnp
from jax import lax

MODEL_DIM = 4096
NUM_HEADS = 32
HEAD_DIM = 128
FF_DIM = 11008
BATCH_SIZE = 8
SEQ_LENGTH = 512
NUM_LAYERS = 2
NORM_EPS = 1e-6
ROPE_THETA = 500000.0


def setup_inputs(seed: int = 0, part: int = 0) -> dict:
    keys = jax.random.split(jax.random.key(seed), 16)
    part_key = jax.random.fold_in(jax.random.key(seed + 1), part)
    dim_scale = MODEL_DIM ** -0.5
    ff_scale = FF_DIM ** -0.5
    square = (NUM_LAYERS, MODEL_DIM, MODEL_DIM)
    wide = (NUM_LAYERS, MODEL_DIM, FF_DIM)

    def normal_weight(key_w, shape_w, scale_w):
        return (jax.random.normal(key_w, shape_w, jnp.float32) * scale_w).astype(jnp.bfloat16)

    def head_scaled(key_w, key_s):
        weight = jax.random.normal(key_w, (NUM_LAYERS, MODEL_DIM, NUM_HEADS, HEAD_DIM), jnp.float32)
        scales = jnp.exp(jax.random.uniform(key_s, (NUM_LAYERS, 1, NUM_HEADS, 1), jnp.float32, -0.6, 0.6))
        return (weight * scales * dim_scale).reshape(square).astype(jnp.bfloat16)

    def gain(key_g):
        return jax.random.uniform(key_g, (NUM_LAYERS, MODEL_DIM), jnp.float32, 0.5, 1.5)

    x = jax.random.normal(part_key, (BATCH_SIZE, SEQ_LENGTH, MODEL_DIM), jnp.float32)
    return {
        'x': x.astype(jnp.bfloat16),
        'w_query': head_scaled(keys[0], keys[1]),
        'w_key': head_scaled(keys[2], keys[3]),
        'w_value': normal_weight(keys[4], square, dim_scale),
        'w_out': normal_weight(keys[5], square, dim_scale),
        'w_gate': normal_weight(keys[6], wide, dim_scale),
        'w_up': normal_weight(keys[7], wide, dim_scale),
        'w_down': normal_weight(keys[8], (NUM_LAYERS, FF_DIM, MODEL_DIM), ff_scale),
        'q_norm_w': gain(keys[9]),
        'k_norm_w': gain(keys[10]),
        'attn_norm_w': gain(keys[11]),
        'ffn_norm_w': gain(keys[12]),
    }


def rope_tables(seq_len):
    half = HEAD_DIM // 2
    inv_freq = ROPE_THETA ** (-2.0 * jnp.arange(half, dtype=jnp.float32) / HEAD_DIM)
    angles = jnp.arange(seq_len, dtype=jnp.float32)[:, None] * inv_freq[None, :]
    return jnp.cos(angles)[:, None, :], jnp.sin(angles)[:, None, :]


def apply_rope(vals, cos_t, sin_t):
    half = HEAD_DIM // 2
    first = vals[..., :half]
    second = vals[..., half:]
    return jnp.concatenate([first * cos_t - second * sin_t, second * cos_t + first * sin_t], axis=-1)


def rms_scale(vals):
    return lax.rsqrt(jnp.mean(vals * vals, axis=-1, keepdims=True) + NORM_EPS)


def attend_one(operands):
    q_seq, k_seq, v_seq = operands
    seq_len = q_seq.shape[0]
    scores = jnp.einsum('qhd,khd->hqk', q_seq.astype(jnp.float32), k_seq.astype(jnp.float32)) * (HEAD_DIM ** -0.5)
    causal = jnp.arange(seq_len)[:, None] >= jnp.arange(seq_len)[None, :]
    scores = jnp.where(causal[None, :, :], scores, -jnp.inf)
    attn_probs = jax.nn.softmax(scores, axis=-1).astype(jnp.bfloat16)
    result = jnp.einsum('hqk,khd->qhd', attn_probs.astype(jnp.float32), v_seq.astype(jnp.float32))
    return result.astype(jnp.bfloat16)


def layer_step(hidden, weights):
    w_query, w_key, w_value, w_out, w_gate, w_up, w_down, q_gain, k_gain, attn_gain, ffn_gain = weights
    batch, seq_len, width = hidden.shape
    flat = hidden.reshape(batch * seq_len, width)
    head_shape = (batch, seq_len, NUM_HEADS, HEAD_DIM)
    cos_t, sin_t = rope_tables(seq_len)
    q_raw = jnp.dot(flat, w_query, preferred_element_type=jnp.float32)
    k_raw = jnp.dot(flat, w_key, preferred_element_type=jnp.float32)
    values = jnp.dot(flat, w_value, preferred_element_type=jnp.float32).astype(jnp.bfloat16).reshape(head_shape)
    queries = apply_rope((q_raw * rms_scale(q_raw) * q_gain).reshape(head_shape), cos_t, sin_t).astype(jnp.bfloat16)
    keys_rot = apply_rope((k_raw * rms_scale(k_raw) * k_gain).reshape(head_shape), cos_t, sin_t).astype(jnp.bfloat16)
    attended = lax.map(attend_one, (queries, keys_rot, values))
    a_out = jnp.dot(attended.reshape(batch * seq_len, width), w_out, preferred_element_type=jnp.float32)
    a_out = a_out.astype(jnp.bfloat16).astype(jnp.float32)
    h_new = (flat.astype(jnp.float32) + a_out * rms_scale(a_out) * attn_gain).astype(jnp.bfloat16)
    gate = jnp.dot(h_new, w_gate, preferred_element_type=jnp.float32)
    up_val = jnp.dot(h_new, w_up, preferred_element_type=jnp.float32)
    hidden_act = (jax.nn.silu(gate) * up_val).astype(jnp.bfloat16)
    m_out = jnp.dot(hidden_act, w_down, preferred_element_type=jnp.float32)
    m_out = m_out.astype(jnp.bfloat16).astype(jnp.float32)
    result = (h_new.astype(jnp.float32) + m_out * rms_scale(m_out) * ffn_gain).astype(jnp.bfloat16)
    return result.reshape(batch, seq_len, width), (keys_rot, values)


def reference(x, w_query, w_key, w_value, w_out, w_gate, w_up, w_down, q_norm_w, k_norm_w, attn_norm_w, ffn_norm_w):
    stacked = (w_query, w_key, w_value, w_out, w_gate, w_up, w_down, q_norm_w, k_norm_w, attn_norm_w, ffn_norm_w)
    y, caches = lax.scan(layer_step, x, stacked)
    return y, caches[0], caches[1]
```

```python
import jax
import jax.numpy as jnp
from jax import lax
from jax.experimental import pallas as pl
from jax.experimental.pallas import tpu as pltpu
from jax.sharding import PartitionSpec as P

HEAD_DIM = 128
NORM_EPS = 1e-6
ROPE_THETA = 500000.0
MESH = pl.DeviceIdType.MESH
BF16 = jnp.bfloat16
F32 = jnp.float32


def rope_tables(seq_len):
    half = HEAD_DIM // 2
    inv_freq = ROPE_THETA ** (-2.0 * jnp.arange(half, dtype=F32) / HEAD_DIM)
    angles = jnp.arange(seq_len, dtype=F32)[:, None] * inv_freq[None, :]
    cos_t, sin_t = jnp.cos(angles), jnp.sin(angles)
    return jnp.concatenate([cos_t, cos_t], axis=-1), jnp.concatenate([-sin_t, sin_t], axis=-1)


def layers_kernel(n_f, n_t, n_layers, *refs):
    (x_in, wq, wk, wv, wo, wg, wu, wd, gq, gk, gains, cos_ref, sin_ref) = refs[:13]
    y_out, k_out, v_out = refs[13:16]
    bufs = refs[16:16 + 5 * n_layers]
    (hid, acc_g, acc_u, kbuf, vbuf, obuf, act, part, full, r1, r2, sqbuf, gbuf,
     wb_qkv, wb_o, wb_gu, wb_d,
     unit_recv, unit_send, ld_sem, ar_recv, ar_send, sq_recv, sq_send, g_recv, g_send, io_sem) = refs[16 + 5 * n_layers:]

    f = lax.axis_index('fsdp')
    t = lax.axis_index('tp')
    tokens, width = hid.shape
    blk = width // n_f
    local_heads = kbuf.shape[1] // HEAD_DIM
    right = lax.rem(f + 2, n_f)
    left = lax.rem(f + n_f - 2, n_f)
    far = lax.rem(f + n_f // 2, n_f)
    mate = f + 1 - 2 * lax.rem(f, 2)
    t_a = t + 1 - 2 * lax.rem(t, 2)
    t_b = n_t - 1 - t
    key_a = lax.rem((t + 1) // 2, 2)
    key_b = t // 2

    barrier = pltpu.get_barrier_semaphore()
    for d in range(1, n_f):
        pl.semaphore_signal(barrier, inc=1, device_id={'fsdp': lax.rem(f + d, n_f)}, device_id_type=MESH)
    for d in range(1, n_t):
        pl.semaphore_signal(barrier, inc=1, device_id={'tp': lax.rem(t + d, n_t)}, device_id_type=MESH)
    pl.semaphore_wait(barrier, n_f + n_t - 2)

    def rcopy(src, dst, send_sem, recv_sem, dev):
        return pltpu.make_async_remote_copy(src_ref=src, dst_ref=dst, send_sem=send_sem, recv_sem=recv_sem,
                                            device_id=dev, device_id_type=MESH)

    units = []
    for layer in range(n_layers):
        b = bufs[5 * layer:5 * layer + 5]
        units.append((b[0], [wq.at[layer], wk.at[layer], wv.at[layer]]))
        units.append((b[1], [wo.at[layer]]))
        units.append((b[2], [wg.at[layer]]))
        units.append((b[3], [wu.at[layer]]))
        units.append((b[4], [wd.at[layer]]))
    n_units = len(units)

    def wait_bytes(ref, sem):
        pltpu.make_async_copy(ref, ref, sem).wait()

    def send_own(u):
        buf, srcs = units[u]
        for slot, dev in ((0, right), (1, left), (4, mate)):
            for j, src in enumerate(srcs):
                rcopy(src, buf.at[f, j], unit_send.at[u], unit_recv.at[u, slot], {'fsdp': dev}).start()

    def service(u):
        buf, srcs = units[u]
        half = buf.shape[2] // 2
        wait_bytes(buf.at[0], unit_recv.at[u, 0])
        src = buf.at[left, :, pl.ds(0, half)]
        rcopy(src, src, unit_send.at[u], unit_recv.at[u, 2], {'fsdp': right}).start()
        src = buf.at[left]
        rcopy(src, src, unit_send.at[u], unit_recv.at[u, 5], {'fsdp': mate}).start()
        wait_bytes(buf.at[0], unit_recv.at[u, 1])
        src = buf.at[right, :, pl.ds(half, half)]
        rcopy(src, src, unit_send.at[u], unit_recv.at[u, 3], {'fsdp': left}).start()
        src = buf.at[right]
        rcopy(src, src, unit_send.at[u], unit_recv.at[u, 6], {'fsdp': mate}).start()
        if u + 2 < n_units:
            send_own(u + 2)

    def finish(u):
        buf, srcs = units[u]
        half = buf.shape[2] // 2
        wait_bytes(buf.at[0, :, pl.ds(0, half)], unit_recv.at[u, 2])
        wait_bytes(buf.at[0, :, pl.ds(0, half)], unit_recv.at[u, 3])
        src = buf.at[far]
        rcopy(src, src, unit_send.at[u], unit_recv.at[u, 7], {'fsdp': mate}).start()
        for slot in (4, 5, 6, 7):
            wait_bytes(buf.at[0], unit_recv.at[u, slot])

    def stream(u, wb, body):
        buf, srcs = units[u]
        for j, src in enumerate(srcs):
            pltpu.make_async_copy(src, wb.at[0, j], ld_sem.at[0]).start()

        def step(i, carry):
            slot = lax.rem(i, 2)
            wait_bytes(wb.at[slot], ld_sem.at[slot])

            @pl.when(i < n_f - 1)
            def _():
                nxt = lax.rem(f + i + 1, n_f)
                pltpu.make_async_copy(buf.at[nxt], wb.at[1 - slot], ld_sem.at[1 - slot]).start()

            body(i, lax.rem(f + i, n_f), slot)
            return carry

        lax.fori_loop(0, n_f, step, 0)

    def accumulate(i, owner, wb, slot, j, acc, col0):
        n_cols = wb.shape[3]
        lhs = hid[:, pl.ds(pl.multiple_of(owner * blk, blk), blk)]
        tile = min(256, n_cols)

        def one(cols_w, cols_a):
            val = jnp.dot(lhs, wb[slot, j, :, cols_w], preferred_element_type=F32)

            @pl.when(i == 0)
            def _():
                acc[:, cols_a] = val

            @pl.when(i > 0)
            def _():
                acc[:, cols_a] += val

        def cols(n, carry):
            off = pl.multiple_of(n * tile, tile)
            one(pl.ds(off, tile), pl.ds(pl.multiple_of(col0 + off, 128), tile))
            return carry

        whole = n_cols // tile
        lax.fori_loop(0, whole, cols, 0)
        rest = n_cols - whole * tile
        if rest:
            one(pl.ds(whole * tile, rest), pl.ds(col0 + whole * tile, rest))

    rows = min(128, tokens)

    def by_rows(body):
        def step(i, carry):
            body(pl.ds(pl.multiple_of(i * rows, rows), rows))
            return carry

        lax.fori_loop(0, tokens // rows, step, 0)

    quarter = width // 4
    eighth = width // 8

    def tp_sum():
        def cols(start, size):
            return pl.ds(pl.multiple_of(start, eighth), size)

        def send(k, src, dst, dev):
            copy = rcopy(src, dst, ar_send.at[k], ar_recv.at[k], {'tp': dev})
            copy.start()
            return copy

        h2 = width // 2
        keep1, keep2 = key_a * quarter, h2 + key_b * quarter
        c0 = send(0, part.at[:, cols((1 - key_a) * quarter, quarter)], r1.at[0], t_a)
        c1 = send(1, part.at[:, cols(h2 + (1 - key_b) * quarter, quarter)], r1.at[1], t_b)

        def add(dst, dst_start, src_start, other, size):
            def body(rs):
                dst[rs, cols(dst_start, size)] = (part[rs, cols(src_start, size)].astype(F32)
                                                  + other[rs, :].astype(F32)).astype(BF16)
            by_rows(body)

        c0.wait_recv()
        add(part, keep1, keep1, r1.at[0], quarter)
        c2 = send(2, part.at[:, cols(keep1 + (1 - key_b) * eighth, eighth)], r2.at[0], t_b)
        c1.wait_recv()
        add(part, keep2, keep2, r1.at[1], quarter)
        c3 = send(3, part.at[:, cols(keep2 + (1 - key_a) * eighth, eighth)], r2.at[1], t_a)
        c2.wait_recv()
        fin1 = keep1 + key_b * eighth
        add(full, fin1, fin1, r2.at[0], eighth)
        c4 = send(4, full.at[:, cols(fin1, eighth)], full.at[:, cols(fin1, eighth)], t_b)
        c3.wait_recv()
        fin2 = keep2 + key_a * eighth
        add(full, fin2, fin2, r2.at[1], eighth)
        c5 = send(5, full.at[:, cols(fin2, eighth)], full.at[:, cols(fin2, eighth)], t_a)
        c4.wait_recv()
        c6 = send(6, full.at[:, cols(keep1, quarter)], full.at[:, cols(keep1, quarter)], t_a)
        c5.wait_recv()
        c7 = send(7, full.at[:, cols(keep2, quarter)], full.at[:, cols(keep2, quarter)], t_b)
        c6.wait_recv()
        c7.wait_recv()
        for c in (c0, c1, c2, c3, c4, c5, c6, c7):
            c.wait_send()

    nrows = min(32, tokens)

    def add_norm(row):
        def step(i, carry):
            rs = pl.ds(pl.multiple_of(i * nrows, nrows), nrows)
            vals = full[rs, :].astype(F32)
            scale = lax.rsqrt(jnp.sum(vals * vals, axis=-1, keepdims=True) / width + NORM_EPS)
            for s in range(n_f):
                cs = pl.ds(s * blk, blk)
                gain = gbuf[s, row:row + 1, :]
                hid[rs, cs] = (hid[rs, cs].astype(F32) + full[rs, cs].astype(F32) * scale * gain).astype(BF16)
            return carry

        lax.fori_loop(0, tokens // nrows, step, 0)

    def qkv_stage(layer, u):
        def body(i, owner, slot):
            accumulate(i, owner, wb_qkv, slot, 0, acc_g, 0)
            accumulate(i, owner, wb_qkv, slot, 1, acc_g, wb_qkv.shape[3])
            accumulate(i, owner, wb_qkv, slot, 2, acc_u, 0)

        stream(u, wb_qkv, body)

    def attention_stage(layer):
        hw = local_heads * HEAD_DIM
        first_half = lax.broadcasted_iota(jnp.int32, (rows, 128), 1) < 64

        def squares(rs):
            q_all = acc_g[rs, pl.ds(0, hw)]
            k_all = acc_g[rs, pl.ds(hw, hw)]
            sq = jnp.sum(q_all * q_all, axis=-1, keepdims=True)
            sk = jnp.sum(k_all * k_all, axis=-1, keepdims=True)
            sqbuf[layer, 0, rs, :] = jnp.where(first_half, sq, sk)

        by_rows(squares)
        copies = []
        for d in range(1, n_t):
            c = rcopy(sqbuf.at[layer, 0], sqbuf.at[layer, d], sq_send.at[layer, d - 1], sq_recv.at[layer, d - 1],
                      {'tp': lax.rem(t + d, n_t)})
            c.start()
            copies.append(c)
        for c in copies:
            c.wait_recv()
        for c in copies:
            c.wait_send()

        def total(rs):
            parts = [sqbuf[layer, lax.rem(t + n_t - dev, n_t), rs, :] for dev in range(n_t)]
            tot = parts[0]
            for p in parts[1:]:
                tot = tot + p
            sqbuf[layer, 0, rs, :] = lax.rsqrt(tot / width + NORM_EPS)

        by_rows(total)

        def head(h, carry):
            cs = pl.ds(pl.multiple_of(h * HEAD_DIM, HEAD_DIM), HEAD_DIM)
            ck = pl.ds(pl.multiple_of(hw + h * HEAD_DIM, HEAD_DIM), HEAD_DIM)
            cos_t, sin_t = cos_ref[...], sin_ref[...]

            def rope(v):
                return v * cos_t + pltpu.roll(v, HEAD_DIM // 2, 1) * sin_t

            inv = sqbuf[layer, 0, :, :]
            qh = rope(acc_g[:, cs] * inv[:, 0:1] * gq[layer:layer + 1, cs]).astype(BF16)
            kbuf[:, cs] = rope(acc_g[:, ck] * inv[:, 64:65] * gk[layer:layer + 1, cs]).astype(BF16)
            vbuf[:, cs] = acc_u[:, cs].astype(BF16)
            qb = min(256, tokens)
            for i in range(tokens // qb):
                end = (i + 1) * qb
                s = lax.dot_general(qh[i * qb:end], kbuf[0:end, cs], (((1,), (1,)), ((), ())),
                                    preferred_element_type=F32) * (HEAD_DIM ** -0.5)
                keep = (lax.broadcasted_iota(jnp.int32, (qb, end), 0) + i * qb
                        >= lax.broadcasted_iota(jnp.int32, (qb, end), 1))
                s = jnp.where(keep, s, -jnp.inf)
                e = jnp.exp(s - jnp.max(s, axis=-1, keepdims=True))
                p = (e / jnp.sum(e, axis=-1, keepdims=True)).astype(BF16)
                obuf[i * qb:end, cs] = jnp.dot(p, vbuf[0:end, cs], preferred_element_type=F32).astype(BF16)
            return carry

        lax.fori_loop(0, local_heads, head, 0)
        ck = pltpu.make_async_copy(kbuf, k_out.at[layer], io_sem.at[0])
        cv = pltpu.make_async_copy(vbuf, v_out.at[layer], io_sem.at[1])
        ck.start()
        cv.start()
        return ck, cv

    def wide_stage(u, lhs, wb):
        def body(i, owner, slot):
            val = jnp.dot(lhs[...], wb[slot, 0], preferred_element_type=F32)
            part[:, pl.ds(pl.multiple_of(owner * blk, blk), blk)] = val.astype(BF16)

        stream(u, wb, body)

    def act_stage():
        def body(rs):
            g = acc_g[rs, :]
            act[rs, :] = (g / (1.0 + jnp.exp(-g)) * acc_u[rs, :]).astype(BF16)

        by_rows(body)

    send_own(0)
    send_own(1)
    load_x = pltpu.make_async_copy(x_in, hid, io_sem.at[2])
    load_x.start()
    gbuf[f] = gains[...]
    for d in range(1, n_f):
        rcopy(gains, gbuf.at[f], g_send, g_recv, {'fsdp': lax.rem(f + d, n_f)}).start()
    load_x.wait()
    wait_bytes(gbuf.at[pl.ds(0, n_f - 1)], g_recv)
    wait_bytes(gbuf.at[pl.ds(0, n_f - 1)], g_send)
    service(0)

    def ready(u):
        if u + 1 < n_units:
            service(u + 1)
        finish(u)

    for layer in range(n_layers):
        u = 5 * layer
        ready(u)
        qkv_stage(layer, u)
        ck, cv = attention_stage(layer)
        ready(u + 1)
        wide_stage(u + 1, obuf, wb_o)
        tp_sum()
        add_norm(2 * layer)
        ck.wait()
        cv.wait()
        ready(u + 2)
        stream(u + 2, wb_gu, lambda i, owner, slot: accumulate(i, owner, wb_gu, slot, 0, acc_g, 0))
        ready(u + 3)
        stream(u + 3, wb_gu, lambda i, owner, slot: accumulate(i, owner, wb_gu, slot, 0, acc_u, 0))
        act_stage()
        ready(u + 4)
        wide_stage(u + 4, act, wb_d)
        tp_sum()
        add_norm(2 * layer + 1)

    store_y = pltpu.make_async_copy(hid, y_out, io_sem.at[2])
    store_y.start()
    for u in range(n_units):
        wait_bytes(units[u][0].at[pl.ds(0, 7)], unit_send.at[u])
    store_y.wait()


def solution(mesh):
    batch_axes = ('dp', 'fsdp')
    act_spec = P(batch_axes, None, None)
    in_cols = P(None, 'fsdp', 'tp')
    in_rows = P(None, 'tp', 'fsdp')
    tp_gain = P(None, 'tp')
    fsdp_gain = P(None, 'fsdp')
    cache_spec = P(None, batch_axes, None, 'tp', None)
    n_f, n_t = mesh.shape['fsdp'], mesh.shape['tp']

    def local_layers(x, w_query, w_key, w_value, w_out, w_gate, w_up, w_down, q_norm_w, k_norm_w, attn_norm_w, ffn_norm_w):
        batch, seq_len, width = x.shape
        n_layers, shard, hw = w_query.shape
        ff = w_gate.shape[2]
        tokens = batch * seq_len
        gains = jnp.stack([attn_norm_w, ffn_norm_w], axis=1).reshape(2 * n_layers, shard)
        gain_rows = -(-2 * n_layers // 8) * 8
        gains = jnp.pad(gains, ((0, gain_rows - 2 * n_layers), (0, 0)))
        cos_t, sin_t = rope_tables(seq_len)
        hbm = pl.BlockSpec(memory_space=pl.ANY)
        vmem = pl.BlockSpec(memory_space=pltpu.VMEM)
        layer_bufs = [jax.ShapeDtypeStruct((n_f, 3, shard, hw), BF16), jax.ShapeDtypeStruct((n_f, 1, hw, shard), BF16),
                      jax.ShapeDtypeStruct((n_f, 1, shard, ff), BF16), jax.ShapeDtypeStruct((n_f, 1, shard, ff), BF16),
                      jax.ShapeDtypeStruct((n_f, 1, ff, shard), BF16)]
        out_shape = [jax.ShapeDtypeStruct((tokens, width), BF16), jax.ShapeDtypeStruct((n_layers, tokens, hw), BF16),
                     jax.ShapeDtypeStruct((n_layers, tokens, hw), BF16)] + layer_bufs * n_layers
        scratch = [
            pltpu.VMEM((tokens, width), BF16),
            pltpu.VMEM((tokens, ff), F32),
            pltpu.VMEM((tokens, ff), F32),
            pltpu.VMEM((tokens, hw), BF16),
            pltpu.VMEM((tokens, hw), BF16),
            pltpu.VMEM((tokens, hw), BF16),
            pltpu.VMEM((tokens, ff), BF16),
            pltpu.VMEM((tokens, width), BF16),
            pltpu.VMEM((tokens, width), BF16),
            pltpu.VMEM((2, tokens, width // 4), BF16),
            pltpu.VMEM((2, tokens, width // 8), BF16),
            pltpu.VMEM((n_layers, n_t, tokens, 128), F32),
            pltpu.VMEM((n_f, gain_rows, shard), F32),
            pltpu.VMEM((2, 3, shard, hw), BF16),
            pltpu.VMEM((2, 1, hw, shard), BF16),
            pltpu.VMEM((2, 1, shard, ff), BF16),
            pltpu.VMEM((2, 1, ff, shard), BF16),
            pltpu.SemaphoreType.DMA((5 * n_layers, 8)),
            pltpu.SemaphoreType.DMA((5 * n_layers,)),
            pltpu.SemaphoreType.DMA((2,)),
            pltpu.SemaphoreType.DMA((8,)),
            pltpu.SemaphoreType.DMA((8,)),
            pltpu.SemaphoreType.DMA((n_layers, n_t - 1)),
            pltpu.SemaphoreType.DMA((n_layers, n_t - 1)),
            pltpu.SemaphoreType.DMA,
            pltpu.SemaphoreType.DMA,
            pltpu.SemaphoreType.DMA((3,)),
        ]
        outs = pl.pallas_call(
            lambda *refs: layers_kernel(n_f, n_t, n_layers, *refs),
            name='layers',
            out_shape=out_shape,
            in_specs=[hbm] * 8 + [vmem] * 5,
            out_specs=[hbm] * len(out_shape),
            scratch_shapes=scratch,
            compiler_params=pltpu.CompilerParams(collective_id=0, has_side_effects=True, vmem_limit_bytes=66 * 1000 * 1000),
        )(x.reshape(tokens, width), w_query, w_key, w_value, w_out, w_gate, w_up, w_down,
          q_norm_w, k_norm_w, gains, cos_t, sin_t)
        cache_shape = (n_layers, batch, seq_len, hw // HEAD_DIM, HEAD_DIM)
        return outs[0].reshape(batch, seq_len, width), outs[1].reshape(cache_shape), outs[2].reshape(cache_shape)

    return jax.shard_map(local_layers, mesh=mesh,
                         in_specs=(act_spec, in_cols, in_cols, in_cols, in_rows, in_cols, in_cols, in_rows,
                                   tp_gain, tp_gain, fsdp_gain, fsdp_gain),
                         out_specs=(act_spec, cache_spec, cache_spec), check_vma=False)
```

```python
import jax
import jax.numpy as jnp
from jax import lax
from jax.experimental import pallas as pl
from jax.experimental.pallas import tpu as pltpu
from jax.sharding import PartitionSpec as P

HEAD_DIM = 128
NORM_EPS = 1e-6
ROPE_THETA = 500000.0
MESH = pl.DeviceIdType.MESH
BF16 = jnp.bfloat16
F32 = jnp.float32


def rope_tables(seq_len):
    half = HEAD_DIM // 2
    inv_freq = ROPE_THETA ** (-2.0 * jnp.arange(half, dtype=F32) / HEAD_DIM)
    angles = jnp.arange(seq_len, dtype=F32)[:, None] * inv_freq[None, :]
    cos_t, sin_t = jnp.cos(angles), jnp.sin(angles)
    return jnp.concatenate([cos_t, cos_t], axis=-1), jnp.concatenate([-sin_t, sin_t], axis=-1)


def layers_kernel(n_f, n_t, n_layers, *refs):
    (x_in, wq, wk, wv, wo, wg, wu, wd, gq, gk, gains, cos_ref, sin_ref) = refs[:13]
    y_out, k_out, v_out = refs[13:16]
    bufs = refs[16:16 + 5 * n_layers]
    (hid, acc_g, acc_u, kbuf, vbuf, obuf, act, part, full, r1, r2, pr, sqbuf, invbuf, gbuf,
     wb_qkv, wb_gu, wb_d,
     unit_recv, unit_send, ld_sem, ex_recv, ex_send, sq_recv, sq_send, g_recv, g_send, io_sem) = refs[16 + 5 * n_layers:]

    f = lax.axis_index('fsdp')
    t = lax.axis_index('tp')
    tokens, width = full.shape
    blk = width // n_f
    hw = kbuf.shape[1]
    local_heads = hw // HEAD_DIM
    ff_half = act.shape[1]
    own_rows, pair_rows = pl.ds(0, tokens), pl.ds(tokens, tokens)

    chip = f // 2
    core = lax.rem(f, 2)
    last_chip = n_f // 2 - 1
    mate = f + 1 - 2 * core
    near = f + 2 - 4 * lax.rem(chip, 2)
    pair = (last_chip - chip) * 2 + core
    near_pair = (last_chip - near // 2) * 2 + core
    cls = chip // 2
    t_a = t + 1 - 2 * lax.rem(t, 2)
    t_b = n_t - 1 - t
    key_a = lax.rem((t + 1) // 2, 2)
    key_b = t // 2

    barrier = pltpu.get_barrier_semaphore()
    for d in range(1, n_f):
        pl.semaphore_signal(barrier, inc=1, device_id={'fsdp': lax.rem(f + d, n_f)}, device_id_type=MESH)
    for d in range(1, n_t):
        pl.semaphore_signal(barrier, inc=1, device_id={'tp': lax.rem(t + d, n_t)}, device_id_type=MESH)
    pl.semaphore_wait(barrier, n_f + n_t - 2)

    def rcopy(src, dst, send_sem, recv_sem, dev):
        return pltpu.make_async_remote_copy(src_ref=src, dst_ref=dst, send_sem=send_sem, recv_sem=recv_sem,
                                            device_id=dev, device_id_type=MESH)

    def half_cols(which):
        return pl.ds(pl.multiple_of(which * ff_half, 128), ff_half)

    units = {}
    order = []
    for layer in range(n_layers):
        b = bufs[5 * layer:5 * layer + 5]
        units['q', layer] = (b[0], [wq.at[layer], wk.at[layer], wv.at[layer]], None)
        units['o', layer] = (b[1], [wo.at[layer]], None)
        units['g', layer] = (b[2], [wg.at[layer, :, half_cols(cls)]], wg.at[layer, :, half_cols(1 - cls)])
        units['u', layer] = (b[3], [wu.at[layer, :, half_cols(cls)]], wu.at[layer, :, half_cols(1 - cls)])
        units['d', layer] = (b[4], [wd.at[layer, half_cols(cls)]], wd.at[layer, half_cols(1 - cls)])
        first = ['q', 'o'] if layer == 0 else ['o', 'q']
        order += [(name, layer) for name in first + ['g', 'u', 'd']]
    n_units = len(order)
    place = {unit: i for i, unit in enumerate(order)}

    def wait_bytes(ref, sem):
        pltpu.make_async_copy(ref, ref, sem).wait()

    def send_own(u):
        buf, srcs, other = units[order[u]]
        for slot, dev in ((1, near), (0, pair), (4, mate)):
            for j, src in enumerate(srcs):
                if slot == 0 and other is not None:
                    src = other
                rcopy(src, buf.at[f, j], unit_send.at[u], unit_recv.at[u, slot], {'fsdp': dev}).start()

    def split(u):
        rows = units[order[u]][0].shape[2]
        if order[u][0] in ('g', 'u', 'd'):
            return rows
        return rows // 2 if u == 0 else rows // 8 * 3

    def pass_on(u, src, slot, dev):
        rcopy(src, src, unit_send.at[u], unit_recv.at[u, slot], {'fsdp': dev}).start()

    def service(unit):
        u = place[unit]
        buf = units[unit][0]
        rows, cut = buf.shape[2], split(u)
        wait_bytes(buf.at[0], unit_recv.at[u, 0])
        pass_on(u, buf.at[pair, :, pl.ds(0, cut)], 2, near)
        pass_on(u, buf.at[pair], 5, mate)
        wait_bytes(buf.at[0], unit_recv.at[u, 1])
        if cut < rows:
            pass_on(u, buf.at[near, :, pl.ds(cut, rows - cut)], 3, pair)
        pass_on(u, buf.at[near], 6, mate)
        if u + 2 < n_units:
            send_own(u + 2)

    def finish(unit):
        u = place[unit]
        buf = units[unit][0]
        rows, cut = buf.shape[2], split(u)
        wait_bytes(buf.at[0, :, pl.ds(0, cut)], unit_recv.at[u, 2])
        if cut < rows:
            wait_bytes(buf.at[0, :, pl.ds(cut, rows - cut)], unit_recv.at[u, 3])
        pass_on(u, buf.at[near_pair], 7, mate)
        for slot in (4, 5, 6, 7):
            wait_bytes(buf.at[0], unit_recv.at[u, slot])

    def stream(unit, wb, body):
        buf, srcs, _ = units[unit]
        for j, src in enumerate(srcs):
            pltpu.make_async_copy(src, wb.at[0, j], ld_sem.at[0]).start()

        def step(i, carry):
            slot = lax.rem(i, 2)
            wait_bytes(wb.at[slot], ld_sem.at[slot])

            @pl.when(i < n_f - 1)
            def _():
                nxt = lax.rem(f + i + 1, n_f)
                pltpu.make_async_copy(buf.at[nxt], wb.at[1 - slot], ld_sem.at[1 - slot]).start()

            body(i, lax.rem(f + i, n_f), slot)
            return carry

        lax.fori_loop(0, n_f, step, 0)

    def accumulate(i, owner, wb, slot, j, lhs_rows, acc, acc_rows):
        n_cols = wb.shape[3]
        lhs = hid[lhs_rows, pl.ds(pl.multiple_of(owner * blk, blk), blk)]
        tile = min(256, n_cols)

        def one(cols_w):
            val = jnp.dot(lhs, wb[slot, j, :, cols_w], preferred_element_type=F32)

            @pl.when(i == 0)
            def _():
                acc[acc_rows, cols_w] = val

            @pl.when(i > 0)
            def _():
                acc[acc_rows, cols_w] += val

        def cols(n, carry):
            one(pl.ds(pl.multiple_of(n * tile, tile), tile))
            return carry

        whole = n_cols // tile
        lax.fori_loop(0, whole, cols, 0)
        rest = n_cols - whole * tile
        if rest:
            one(pl.ds(whole * tile, rest))

    rows = min(128, tokens)

    def by_rows(body, total=tokens):
        def step(i, carry):
            body(i * rows)
            return carry

        lax.fori_loop(0, total // rows, step, 0)

    def chunk(start):
        return pl.ds(pl.multiple_of(start, rows), rows)

    quarter, eighth, half = width // 4, width // 8, width // 2
    keep1, keep2 = key_a * quarter, half + key_b * quarter
    fin1, fin2 = keep1 + key_b * eighth, keep2 + key_a * eighth

    def cols(start, size):
        return pl.ds(pl.multiple_of(start, eighth), size)

    def send(k, src, dst, dev):
        copy = rcopy(src, dst, ex_send.at[k], ex_recv.at[k], dev)
        copy.start()
        return copy

    def add(dst, dst_row0, row0, start, size, others):
        def body(r):
            val = part[chunk(row0 + r), cols(start, size)].astype(F32)
            for other in others:
                val = val + other[chunk(r), :].astype(F32)
            dst[chunk(dst_row0 + r), cols(start, size)] = val.astype(BF16)

        by_rows(body)

    def scatter_begin(g):
        rs = pl.ds(g * tokens, tokens)
        return [send(8 * g, part.at[rs, cols((1 - key_a) * quarter, quarter)], r1.at[2 * g], {'tp': t_a}),
                send(8 * g + 1, part.at[rs, cols(half + (1 - key_b) * quarter, quarter)], r1.at[2 * g + 1], {'tp': t_b})]

    def scatter_next(g, cs):
        rs, row0 = pl.ds(g * tokens, tokens), g * tokens
        cs[0].wait_recv()
        add(part, row0, row0, keep1, quarter, [r1.at[2 * g]])
        cs.append(send(8 * g + 2, part.at[rs, cols(keep1 + (1 - key_b) * eighth, eighth)], r2.at[2 * g], {'tp': t_b}))
        cs[1].wait_recv()
        add(part, row0, row0, keep2, quarter, [r1.at[2 * g + 1]])
        cs.append(send(8 * g + 3, part.at[rs, cols(keep2 + (1 - key_a) * eighth, eighth)], r2.at[2 * g + 1], {'tp': t_a}))

    def spread_first(k, buf, rs, which):
        start, dev = ((fin1, t_b), (fin2, t_a))[which]
        view = buf.at[rs, cols(start, eighth)]
        return send(k + which, view, view, {'tp': dev})

    def spread_next(k, buf, rs, cs):
        cs[0].wait_recv()
        view = buf.at[rs, cols(keep1, quarter)]
        cs.append(send(k + 2, view, view, {'tp': t_a}))
        cs[1].wait_recv()
        view = buf.at[rs, cols(keep2, quarter)]
        cs.append(send(k + 3, view, view, {'tp': t_b}))

    def drain(cs):
        for c in cs:
            c.wait_send()

    nrows = min(32, tokens)

    def add_norm(row):
        def step(i, carry):
            rs = pl.ds(pl.multiple_of(i * nrows, nrows), nrows)
            vals = full[rs, :].astype(F32)
            scale = lax.rsqrt(jnp.sum(vals * vals, axis=-1, keepdims=True) / width + NORM_EPS)
            for s in range(n_f):
                cs = pl.ds(s * blk, blk)
                gain = gbuf[s, row:row + 1, :]
                hid[rs, cs] = (hid[rs, cs].astype(F32) + full[rs, cs].astype(F32) * scale * gain).astype(BF16)
            return carry

        lax.fori_loop(0, tokens // nrows, step, 0)

    def qkv_stage(layer):
        def body(i, owner, slot):
            accumulate(i, owner, wb_qkv, slot, 0, own_rows, acc_g, own_rows)
            accumulate(i, owner, wb_qkv, slot, 1, own_rows, acc_g, pair_rows)
            accumulate(i, owner, wb_qkv, slot, 2, own_rows, acc_u, own_rows)

        stream(('q', layer), wb_qkv, body)

    n_blocks = tokens // 128

    def attention_stage(layer):
        lane = lax.broadcasted_iota(jnp.int32, (128, 128), 1)
        eye = lax.broadcasted_iota(jnp.int32, (128, 128), 0) == lane

        for which in range(2):
            for b in range(n_blocks):
                vals = acc_g[pl.ds(which * tokens + b * 128, 128), pl.ds(0, hw)]
                col = jnp.sum(vals * vals, axis=-1, keepdims=True)
                row = which * n_blocks + b
                sqbuf[layer, 0, row:row + 1, :] = jnp.sum(jnp.where(eye, col, 0.0), axis=0, keepdims=True)
        copies = []
        for d in range(1, n_t):
            c = rcopy(sqbuf.at[layer, 0], sqbuf.at[layer, d], sq_send.at[layer, d - 1], sq_recv.at[layer, d - 1],
                      {'tp': lax.rem(t + d, n_t)})
            c.start()
            copies.append(c)
        for c in copies:
            c.wait_recv()
        drain(copies)
        tot = sqbuf[layer, 0]
        for d in range(1, n_t):
            tot = tot + sqbuf[layer, d]
        inv_rows = lax.rsqrt(tot / width + NORM_EPS)
        for b in range(n_blocks):
            inv_q = jnp.sum(jnp.where(eye, inv_rows[b:b + 1, :], 0.0), axis=1, keepdims=True)
            inv_k = jnp.sum(jnp.where(eye, inv_rows[n_blocks + b:n_blocks + b + 1, :], 0.0), axis=1, keepdims=True)
            invbuf[pl.ds(b * 128, 128), :] = jnp.where(lane < 64, inv_q, inv_k)

        def head(h, carry):
            cs = pl.ds(pl.multiple_of(h * HEAD_DIM, HEAD_DIM), HEAD_DIM)
            cos_t, sin_t = cos_ref[...], sin_ref[...]

            def rope(v):
                return v * cos_t + pltpu.roll(v, HEAD_DIM // 2, 1) * sin_t

            inv = invbuf[...]
            qh = rope(acc_g[own_rows, cs] * inv[:, 0:1] * gq[layer:layer + 1, cs]).astype(BF16)
            kbuf[:, cs] = rope(acc_g[pair_rows, cs] * inv[:, 64:65] * gk[layer:layer + 1, cs]).astype(BF16)
            vbuf[:, cs] = acc_u[own_rows, cs].astype(BF16)
            qb = min(256, tokens)
            for i in range(tokens // qb):
                end = (i + 1) * qb
                s = lax.dot_general(qh[i * qb:end], kbuf[0:end, cs], (((1,), (1,)), ((), ())),
                                    preferred_element_type=F32) * (HEAD_DIM ** -0.5)
                keep = (lax.broadcasted_iota(jnp.int32, (qb, end), 0) + i * qb
                        >= lax.broadcasted_iota(jnp.int32, (qb, end), 1))
                s = jnp.where(keep, s, -jnp.inf)
                e = jnp.exp(s - jnp.max(s, axis=-1, keepdims=True))
                p = (e / jnp.sum(e, axis=-1, keepdims=True)).astype(BF16)
                obuf[i * qb:end, cs] = jnp.dot(p, vbuf[0:end, cs], preferred_element_type=F32).astype(BF16)
            return carry

        lax.fori_loop(0, local_heads, head, 0)
        ck = pltpu.make_async_copy(kbuf, k_out.at[layer], io_sem.at[0])
        cv = pltpu.make_async_copy(vbuf, v_out.at[layer], io_sem.at[1])
        ck.start()
        cv.start()
        return ck, cv

    def wide_stage(unit, lhs, out_rows, wb):
        def body(i, owner, slot):
            val = jnp.dot(lhs[...], wb[slot, 0], preferred_element_type=F32)
            part[out_rows, pl.ds(pl.multiple_of(owner * blk, blk), blk)] = val.astype(BF16)

        stream(unit, wb, body)

    def out_stage(layer):
        wide_stage(('o', layer), obuf, own_rows, wb_d.at[:, :, pl.ds(0, hw)])
        cs = scatter_begin(0)
        scatter_next(0, cs)
        cs[2].wait_recv()
        add(full, 0, 0, fin1, eighth, [r2.at[0]])
        cs2 = [spread_first(4, full, own_rows, 0)]
        cs[3].wait_recv()
        add(full, 0, 0, fin2, eighth, [r2.at[1]])
        cs2.append(spread_first(4, full, own_rows, 1))
        spread_next(4, full, own_rows, cs2)
        cs2[2].wait_recv()
        cs2[3].wait_recv()
        drain(cs + cs2)
        add_norm(2 * layer)

    def mlp_stage(layer):
        ex = []
        for k, start in ((16, fin1), (17, fin2)):
            ex.append(send(k, hid.at[own_rows, cols(start, eighth)], hid.at[pair_rows, cols(start, eighth)],
                           {'fsdp': pair}))

        def pass_over(name, acc, rs):
            stream((name, layer), wb_gu, lambda i, owner, slot: accumulate(i, owner, wb_gu, slot, 0, rs, acc, rs))

        service(('u', layer))
        finish(('g', layer))
        pass_over('g', acc_g, own_rows)
        ex[0].wait_recv()
        cs = [spread_first(12, hid, pair_rows, 0)]
        ex[1].wait_recv()
        cs.append(spread_first(12, hid, pair_rows, 1))
        service(('d', layer))
        spread_next(12, hid, pair_rows, cs)
        finish(('u', layer))
        pass_over('u', acc_u, own_rows)
        cs[2].wait_recv()
        cs[3].wait_recv()
        pass_over('g', acc_g, pair_rows)
        pass_over('u', acc_u, pair_rows)
        drain(ex + cs)

        def gate(r):
            g = acc_g[chunk(r), :]
            act[chunk(r), :] = (g / (1.0 + jnp.exp(-g)) * acc_u[chunk(r), :]).astype(BF16)

        by_rows(gate, 2 * tokens)

        finish(('d', layer))
        wide_stage(('d', layer), act, pl.ds(0, 2 * tokens), wb_d)
        cp = scatter_begin(1)
        co = scatter_begin(0)
        scatter_next(1, cp)
        scatter_next(0, co)
        cp[2].wait_recv()
        add(part, tokens, tokens, fin1, eighth, [r2.at[2]])
        ce = [send(18, part.at[pair_rows, cols(fin1, eighth)], pr.at[0], {'fsdp': pair})]
        cp[3].wait_recv()
        add(part, tokens, tokens, fin2, eighth, [r2.at[3]])
        ce.append(send(19, part.at[pair_rows, cols(fin2, eighth)], pr.at[1], {'fsdp': pair}))
        if layer + 1 < n_layers:
            service(('o', layer + 1))
        co[2].wait_recv()
        ce[0].wait_recv()
        add(full, 0, 0, fin1, eighth, [r2.at[0], pr.at[0]])
        cs = [spread_first(4, full, own_rows, 0)]
        co[3].wait_recv()
        ce[1].wait_recv()
        add(full, 0, 0, fin2, eighth, [r2.at[1], pr.at[1]])
        cs.append(spread_first(4, full, own_rows, 1))
        spread_next(4, full, own_rows, cs)
        if layer + 1 < n_layers:
            service(('q', layer + 1))
        cs[2].wait_recv()
        cs[3].wait_recv()
        drain(cp + co + ce + cs)
        add_norm(2 * layer + 1)

    send_own(0)
    send_own(1)
    load_x = pltpu.make_async_copy(x_in, hid.at[own_rows], io_sem.at[2])
    load_x.start()
    gbuf[f] = gains[...]
    for d in range(1, n_f):
        rcopy(gains, gbuf.at[f], g_send, g_recv, {'fsdp': lax.rem(f + d, n_f)}).start()
    load_x.wait()
    wait_bytes(gbuf.at[pl.ds(0, n_f - 1)], g_recv)
    wait_bytes(gbuf.at[pl.ds(0, n_f - 1)], g_send)
    service(('q', 0))
    service(('o', 0))

    for layer in range(n_layers):
        finish(('q', layer))
        qkv_stage(layer)
        ck, cv = attention_stage(layer)
        service(('g', layer))
        finish(('o', layer))
        out_stage(layer)
        ck.wait()
        cv.wait()
        mlp_stage(layer)

    store_y = pltpu.make_async_copy(hid.at[own_rows], y_out, io_sem.at[2])
    store_y.start()
    for u in range(n_units):
        wait_bytes(units[order[u]][0].at[pl.ds(0, 7)], unit_send.at[u])
    store_y.wait()


def solution(mesh):
    batch_axes = ('dp', 'fsdp')
    act_spec = P(batch_axes, None, None)
    in_cols = P(None, 'fsdp', 'tp')
    in_rows = P(None, 'tp', 'fsdp')
    tp_gain = P(None, 'tp')
    fsdp_gain = P(None, 'fsdp')
    cache_spec = P(None, batch_axes, None, 'tp', None)
    n_f, n_t = mesh.shape['fsdp'], mesh.shape['tp']

    def local_layers(x, w_query, w_key, w_value, w_out, w_gate, w_up, w_down, q_norm_w, k_norm_w, attn_norm_w, ffn_norm_w):
        batch, seq_len, width = x.shape
        n_layers, shard, hw = w_query.shape
        ff = w_gate.shape[2]
        tokens = batch * seq_len
        gains = jnp.stack([attn_norm_w, ffn_norm_w], axis=1).reshape(2 * n_layers, shard)
        gain_rows = -(-2 * n_layers // 8) * 8
        gains = jnp.pad(gains, ((0, gain_rows - 2 * n_layers), (0, 0)))
        cos_t, sin_t = rope_tables(seq_len)
        hbm = pl.BlockSpec(memory_space=pl.ANY)
        vmem = pl.BlockSpec(memory_space=pltpu.VMEM)
        ff_half = -(-ff // 256) * 128
        extra = 2 * ff_half - ff
        w_gate = jnp.pad(w_gate, ((0, 0), (0, 0), (0, extra)))
        w_up = jnp.pad(w_up, ((0, 0), (0, 0), (0, extra)))
        w_down = jnp.pad(w_down, ((0, 0), (0, extra), (0, 0)))
        layer_bufs = [jax.ShapeDtypeStruct((n_f, 3, shard, hw), BF16), jax.ShapeDtypeStruct((n_f, 1, hw, shard), BF16),
                      jax.ShapeDtypeStruct((n_f, 1, shard, ff_half), BF16),
                      jax.ShapeDtypeStruct((n_f, 1, shard, ff_half), BF16),
                      jax.ShapeDtypeStruct((n_f, 1, ff_half, shard), BF16)]
        out_shape = [jax.ShapeDtypeStruct((tokens, width), BF16), jax.ShapeDtypeStruct((n_layers, tokens, hw), BF16),
                     jax.ShapeDtypeStruct((n_layers, tokens, hw), BF16)] + layer_bufs * n_layers
        sq_rows = -(-2 * (tokens // 128) // 8) * 8
        scratch = [
            pltpu.VMEM((2 * tokens, width), BF16),
            pltpu.VMEM((2 * tokens, ff_half), F32),
            pltpu.VMEM((2 * tokens, ff_half), F32),
            pltpu.VMEM((tokens, hw), BF16),
            pltpu.VMEM((tokens, hw), BF16),
            pltpu.VMEM((tokens, hw), BF16),
            pltpu.VMEM((2 * tokens, ff_half), BF16),
            pltpu.VMEM((2 * tokens, width), BF16),
            pltpu.VMEM((tokens, width), BF16),
            pltpu.VMEM((4, tokens, width // 4), BF16),
            pltpu.VMEM((4, tokens, width // 8), BF16),
            pltpu.VMEM((2, tokens, width // 8), BF16),
            pltpu.VMEM((n_layers, n_t, sq_rows, 128), F32),
            pltpu.VMEM((tokens, 128), F32),
            pltpu.VMEM((n_f, gain_rows, shard), F32),
            pltpu.VMEM((2, 3, shard, hw), BF16),
            pltpu.VMEM((2, 1, shard, ff_half), BF16),
            pltpu.VMEM((2, 1, ff_half, shard), BF16),
            pltpu.SemaphoreType.DMA((5 * n_layers, 8)),
            pltpu.SemaphoreType.DMA((5 * n_layers,)),
            pltpu.SemaphoreType.DMA((2,)),
            pltpu.SemaphoreType.DMA((20,)),
            pltpu.SemaphoreType.DMA((20,)),
            pltpu.SemaphoreType.DMA((n_layers, n_t - 1)),
            pltpu.SemaphoreType.DMA((n_layers, n_t - 1)),
            pltpu.SemaphoreType.DMA,
            pltpu.SemaphoreType.DMA,
            pltpu.SemaphoreType.DMA((3,)),
        ]
        outs = pl.pallas_call(
            lambda *refs: layers_kernel(n_f, n_t, n_layers, *refs),
            name='layers',
            out_shape=out_shape,
            in_specs=[hbm] * 8 + [vmem] * 5,
            out_specs=[hbm] * len(out_shape),
            scratch_shapes=scratch,
            compiler_params=pltpu.CompilerParams(collective_id=0, has_side_effects=True, vmem_limit_bytes=66 * 1000 * 1000),
        )(x.reshape(tokens, width), w_query, w_key, w_value, w_out, w_gate, w_up, w_down,
          q_norm_w, k_norm_w, gains, cos_t, sin_t)
        cache_shape = (n_layers, batch, seq_len, hw // HEAD_DIM, HEAD_DIM)
        return outs[0].reshape(batch, seq_len, width), outs[1].reshape(cache_shape), outs[2].reshape(cache_shape)

    return jax.shard_map(local_layers, mesh=mesh,
                         in_specs=(act_spec, in_cols, in_cols, in_cols, in_rows, in_cols, in_cols, in_rows,
                                   tp_gain, tp_gain, fsdp_gain, fsdp_gain),
                         out_specs=(act_spec, cache_spec, cache_spec), check_vma=False)
```

```python
import jax
import jax.numpy as jnp
from jax import lax
from jax.experimental import pallas as pl
from jax.experimental.pallas import tpu as pltpu
from jax.sharding import PartitionSpec as P

HEAD_DIM = 128
NORM_EPS = 1e-6
ROPE_THETA = 500000.0
MESH = pl.DeviceIdType.MESH
BF16 = jnp.bfloat16
F32 = jnp.float32


def rope_tables(seq_len):
    half = HEAD_DIM // 2
    inv_freq = ROPE_THETA ** (-2.0 * jnp.arange(half, dtype=F32) / HEAD_DIM)
    angles = jnp.arange(seq_len, dtype=F32)[:, None] * inv_freq[None, :]
    cos_t, sin_t = jnp.cos(angles), jnp.sin(angles)
    return jnp.concatenate([cos_t, cos_t], axis=-1), jnp.concatenate([-sin_t, sin_t], axis=-1)


def layers_kernel(n_f, n_t, n_layers, *refs):
    (x_in, wq, wk, wv, wo, wg, wu, wd, gq, gk, gains, cos_ref, sin_ref) = refs[:13]
    y_out, k_out, v_out = refs[13:16]
    bufs = refs[16:16 + 5 * n_layers]
    (hid, acc, kbuf, vbuf, obuf, act, part, fin, r1, r2, pr, sqbuf, invbuf, gbuf,
     wb_qkv, wb_gu, wb_o, wb_d,
     unit_recv, unit_send, ld_sem, ex_recv, ex_send, sq_recv, sq_send, g_recv, g_send, io_sem) = refs[16 + 5 * n_layers:]

    f = lax.axis_index('fsdp')
    t = lax.axis_index('tp')
    tokens, width = x_in.shape
    blk = width // n_f
    hw = kbuf.shape[1]
    local_heads = hw // HEAD_DIM
    ff_half = act.shape[1]
    own_rows, pair_rows = pl.ds(0, tokens), pl.ds(tokens, tokens)

    chip = f // 2
    core = lax.rem(f, 2)
    last_chip = n_f // 2 - 1
    mate = f + 1 - 2 * core
    near = f + 2 - 4 * lax.rem(chip, 2)
    pair = (last_chip - chip) * 2 + core
    near_pair = (last_chip - near // 2) * 2 + core
    cls = chip // 2
    t_a = t + 1 - 2 * lax.rem(t, 2)
    t_b = n_t - 1 - t
    key_a = lax.rem((t + 1) // 2, 2)
    key_b = t // 2

    barrier = pltpu.get_barrier_semaphore()
    for d in range(1, n_f):
        pl.semaphore_signal(barrier, inc=1, device_id={'fsdp': lax.rem(f + d, n_f)}, device_id_type=MESH)
    for d in range(1, n_t):
        pl.semaphore_signal(barrier, inc=1, device_id={'tp': lax.rem(t + d, n_t)}, device_id_type=MESH)
    pl.semaphore_wait(barrier, n_f + n_t - 2)

    def rcopy(src, dst, send_sem, recv_sem, dev):
        return pltpu.make_async_remote_copy(src_ref=src, dst_ref=dst, send_sem=send_sem, recv_sem=recv_sem,
                                            device_id=dev, device_id_type=MESH)

    def half_rows(which):
        return pl.ds(pl.multiple_of(which * ff_half, 16), ff_half)

    units = {}
    order = []
    for layer in range(n_layers):
        b = bufs[5 * layer:5 * layer + 5]
        units['q', layer] = (b[0], [wq.at[layer], wk.at[layer], wv.at[layer]], None)
        units['o', layer] = (b[1], [wo.at[layer]], None)
        units['g', layer] = (b[2], [wg.at[layer, half_rows(cls)]], wg.at[layer, half_rows(1 - cls)])
        units['u', layer] = (b[3], [wu.at[layer, half_rows(cls)]], wu.at[layer, half_rows(1 - cls)])
        units['d', layer] = (b[4], [wd.at[layer, half_rows(cls)]], wd.at[layer, half_rows(1 - cls)])
        first = ['q', 'o'] if layer == 0 else ['o', 'q']
        order += [(name, layer) for name in first + ['g', 'u', 'd']]
    n_units = len(order)
    place = {unit: i for i, unit in enumerate(order)}

    def wait_bytes(ref, sem):
        pltpu.make_async_copy(ref, ref, sem).wait()

    def send_own(u):
        buf, srcs, other = units[order[u]]
        for slot, dev in ((1, near), (0, pair), (4, mate)):
            for j, src in enumerate(srcs):
                if slot == 0 and other is not None:
                    src = other
                rcopy(src, buf.at[f, j], unit_send.at[u], unit_recv.at[u, slot], {'fsdp': dev}).start()

    def split(u):
        rows = units[order[u]][0].shape[2]
        if order[u][0] in ('g', 'u', 'd'):
            return rows
        return rows // 2 if u == 0 else rows // 8 * 3

    def pass_on(u, src, slot, dev):
        rcopy(src, src, unit_send.at[u], unit_recv.at[u, slot], {'fsdp': dev}).start()

    def service(unit):
        with jax.named_scope('service_%s%d' % unit):
            service_unit(unit)

    def service_unit(unit):
        u = place[unit]
        buf = units[unit][0]
        rows, cut = buf.shape[2], split(u)
        wait_bytes(buf.at[0], unit_recv.at[u, 0])
        pass_on(u, buf.at[pair, :, pl.ds(0, cut)], 2, near)
        pass_on(u, buf.at[pair], 5, mate)
        wait_bytes(buf.at[0], unit_recv.at[u, 1])
        if cut < rows:
            pass_on(u, buf.at[near, :, pl.ds(cut, rows - cut)], 3, pair)
        pass_on(u, buf.at[near], 6, mate)
        if u + 2 < n_units:
            send_own(u + 2)

    def finish(unit):
        with jax.named_scope('finish_%s%d' % unit):
            finish_unit(unit)

    def finish_unit(unit):
        u = place[unit]
        buf = units[unit][0]
        rows, cut = buf.shape[2], split(u)
        wait_bytes(buf.at[0, :, pl.ds(0, cut)], unit_recv.at[u, 2])
        if cut < rows:
            wait_bytes(buf.at[0, :, pl.ds(cut, rows - cut)], unit_recv.at[u, 3])
        pass_on(u, buf.at[near_pair], 7, mate)
        for slot in (4, 5, 6, 7):
            wait_bytes(buf.at[0], unit_recv.at[u, slot])

    def load(unit, j, piece, owner, dst, sem):
        buf, srcs, _ = units[unit]

        @pl.when(owner == f)
        def _():
            pltpu.make_async_copy(srcs[j].at[piece], dst, sem).start()

        @pl.when(owner != f)
        def _():
            pltpu.make_async_copy(buf.at[(owner, j) + piece], dst, sem).start()

    def lanes(start, size):
        return pl.ds(pl.multiple_of(start, size), size)

    def qkv_stage(layer):
        tile = wb_qkv.shape[2]
        n_tiles = hw // tile

        def fetch(j, n, slot):
            for s in range(n_f):
                load(('q', layer), j, (slice(None), lanes(n * tile, tile)), s,
                     wb_qkv.at[slot, pl.ds(s * blk, blk)], ld_sem.at[slot])

        fetch(0, 0, 0)
        for j in range(3):
            def step(n, carry):
                slot = lax.rem(n + j * n_tiles, 2)
                wait_bytes(wb_qkv.at[slot], ld_sem.at[slot])

                @pl.when(n < n_tiles - 1)
                def _():
                    fetch(j, n + 1, 1 - slot)

                if j < 2:
                    @pl.when(n == n_tiles - 1)
                    def _():
                        fetch(j + 1, 0, 1 - slot)

                val = jnp.dot(hid[own_rows, :], wb_qkv[slot], preferred_element_type=F32)
                if j < 2:
                    acc[j, :, lanes(n * tile, tile)] = val
                else:
                    vbuf[:, lanes(n * tile, tile)] = val.astype(BF16)
                return carry

            with jax.named_scope('qkv%d_%d' % (j, layer)):
                lax.fori_loop(0, n_tiles, step, 0)

    gu_tile = min(256, ff_half)
    gu_whole = ff_half // gu_tile
    gu_rest = ff_half - gu_whole * gu_tile

    def gu_fetch(layer, n, size, slot):
        for j, name in enumerate(('g', 'u')):
            for s in range(n_f):
                start = n * gu_tile
                if not isinstance(start, int):
                    start = pl.multiple_of(start, gu_tile)
                load((name, layer), 0, (pl.ds(start, size),), s,
                     wb_gu.at[slot, j, pl.ds(0, size), pl.ds(s * blk, blk)], ld_sem.at[slot])

    def gu_tile_product(size, slot, rs, out_cols):
        lhs = hid[rs, :]
        dims = (((1,), (1,)), ((), ()))
        g = lax.dot_general(lhs, wb_gu[slot, 0, 0:size, :], dims, preferred_element_type=F32)
        up = lax.dot_general(lhs, wb_gu[slot, 1, 0:size, :], dims, preferred_element_type=F32)
        act[rs, out_cols] = (g / (1.0 + jnp.exp(-g)) * up).astype(BF16)

    def gu_tiles(layer, rs, lo, hi):
        def step(n, carry):
            slot = lax.rem(n, 2)
            wait_bytes(wb_gu.at[slot], ld_sem.at[slot])

            @pl.when(n < gu_whole - 1)
            def _():
                gu_fetch(layer, n + 1, gu_tile, 1 - slot)

            if gu_rest and hi == gu_whole:
                @pl.when(n == gu_whole - 1)
                def _():
                    gu_fetch(layer, gu_whole, gu_rest, 1 - slot)

            gu_tile_product(gu_tile, slot, rs, lanes(n * gu_tile, gu_tile))
            return carry

        lax.fori_loop(lo, hi, step, 0)
        if gu_rest and hi == gu_whole:
            slot = gu_whole % 2
            wait_bytes(wb_gu.at[slot, :, pl.ds(0, gu_rest)], ld_sem.at[slot])
            gu_tile_product(gu_rest, slot, rs, pl.ds(gu_whole * gu_tile, gu_rest))

    def wide_segment(g):
        side, kept = lax.rem(g, 2), g // 2
        key = key_a + (key_b - key_a) * side
        return 2 * side + key * kept + (1 - key) * (1 - kept)

    def wide_fetch(unit, wb, g, slot):
        for e in range(2):
            load(unit, 0, (), 2 * wide_segment(g) + e, wb.at[slot, e], ld_sem.at[slot])

    def wide_stage(unit, lhs, out_rows, wb, lo, hi):
        def step(g, carry):
            slot = lax.rem(g, 2)
            wait_bytes(wb.at[slot], ld_sem.at[slot])

            @pl.when(g < 3)
            def _():
                wide_fetch(unit, wb, g + 1, 1 - slot)

            for e in range(2):
                val = jnp.dot(lhs[...], wb[slot, e], preferred_element_type=F32)
                start = (2 * wide_segment(g) + e) * blk
                part[out_rows, pl.ds(pl.multiple_of(start, blk), blk)] = val.astype(BF16)
            return carry

        with jax.named_scope('wide_%s%d' % unit):
            lax.fori_loop(lo, hi, step, 0)

    rows = min(128, tokens)

    def by_rows(body, total=tokens):
        def step(i, carry):
            body(i * rows)
            return carry

        lax.fori_loop(0, total // rows, step, 0)

    def chunk(start):
        return pl.ds(pl.multiple_of(start, rows), rows)

    quarter, eighth, half = width // 4, width // 8, width // 2
    keep1, keep2 = key_a * quarter, half + key_b * quarter
    fin1, fin2 = keep1 + key_b * eighth, keep2 + key_a * eighth

    def cols(start, size):
        return pl.ds(pl.multiple_of(start, eighth), size)

    def send(k, src, dst, dev):
        copy = rcopy(src, dst, ex_send.at[k], ex_recv.at[k], dev)
        copy.start()
        return copy

    def add(row0, start, size, others, dst=None):
        def body(r):
            val = part[chunk(row0 + r), cols(start, size)].astype(F32)
            for other in others:
                val = val + other[chunk(r), :].astype(F32)
            if dst is None:
                part[chunk(row0 + r), cols(start, size)] = val.astype(BF16)
            else:
                dst[chunk(r), :] = val.astype(BF16)

        by_rows(body)

    def scatter_begin(g):
        rs = pl.ds(g * tokens, tokens)
        return [send(8 * g, part.at[rs, cols((1 - key_a) * quarter, quarter)], r1.at[2 * g], {'tp': t_a}),
                send(8 * g + 1, part.at[rs, cols(half + (1 - key_b) * quarter, quarter)], r1.at[2 * g + 1], {'tp': t_b})]

    def scatter_next(g, cs):
        rs, row0 = pl.ds(g * tokens, tokens), g * tokens
        cs[0].wait_recv()
        add(row0, keep1, quarter, [r1.at[2 * g]])
        cs.append(send(8 * g + 2, part.at[rs, cols(keep1 + (1 - key_b) * eighth, eighth)], r2.at[2 * g], {'tp': t_b}))
        cs[1].wait_recv()
        add(row0, keep2, quarter, [r1.at[2 * g + 1]])
        cs.append(send(8 * g + 3, part.at[rs, cols(keep2 + (1 - key_a) * eighth, eighth)], r2.at[2 * g + 1], {'tp': t_a}))

    def spread_first(k, rs, which):
        start, dev = ((fin1, t_b), (fin2, t_a))[which]
        view = hid.at[rs, cols(start, eighth)]
        return send(k + which, view, view, {'tp': dev})

    def spread_next(k, rs, cs):
        cs[0].wait_recv()
        view = hid.at[rs, cols(keep1, quarter)]
        cs.append(send(k + 2, view, view, {'tp': t_a}))
        cs[1].wait_recv()
        view = hid.at[rs, cols(keep2, quarter)]
        cs.append(send(k + 3, view, view, {'tp': t_b}))

    def drain(cs):
        for c in cs:
            c.wait_send()

    n_blocks = tokens // 128
    lane = lax.broadcasted_iota(jnp.int32, (128, 128), 1)
    eye = lax.broadcasted_iota(jnp.int32, (128, 128), 0) == lane

    def to_row(col):
        return jnp.sum(jnp.where(eye, col, 0.0), axis=0, keepdims=True)

    def to_col(row):
        return jnp.sum(jnp.where(eye, row, 0.0), axis=1, keepdims=True)

    def inverse_rms(k):
        copies = []
        for d in range(1, n_t):
            c = rcopy(sqbuf.at[k, 0], sqbuf.at[k, d], sq_send.at[k, d - 1], sq_recv.at[k, d - 1],
                      {'tp': lax.rem(t + d, n_t)})
            c.start()
            copies.append(c)
        with jax.named_scope('squares_%d' % k):
            for c in copies:
                c.wait_recv()
            drain(copies)
        tot = sqbuf[k, 0]
        for d in range(1, n_t):
            tot = tot + sqbuf[k, d]
        return lax.rsqrt(tot / width + NORM_EPS)

    def add_norm(row, k):
        for b in range(n_blocks):
            rs = pl.ds(b * 128, 128)
            a0, a1 = fin[0, rs, :].astype(F32), fin[1, rs, :].astype(F32)
            col = jnp.sum(a0 * a0, axis=-1, keepdims=True) + jnp.sum(a1 * a1, axis=-1, keepdims=True)
            sqbuf[k, 0, b:b + 1, :] = to_row(col)
        inv = inverse_rms(k)
        for b in range(n_blocks):
            rs = pl.ds(b * 128, 128)
            scale = to_col(inv[b:b + 1, :])
            for e, start in ((0, fin1), (1, fin2)):
                gain = gbuf[start // eighth, row:row + 1, :]
                hid[rs, cols(start, eighth)] = (hid[rs, cols(start, eighth)].astype(F32)
                                                + fin[e, rs, :].astype(F32) * scale * gain).astype(BF16)

    def attention_stage(layer):
        for which in range(2):
            for b in range(n_blocks):
                vals = acc[which, pl.ds(b * 128, 128), :]
                row = which * n_blocks + b
                sqbuf[3 * layer, 0, row:row + 1, :] = to_row(jnp.sum(vals * vals, axis=-1, keepdims=True))
        inv_rows = inverse_rms(3 * layer)
        for b in range(n_blocks):
            inv_q = to_col(inv_rows[b:b + 1, :])
            inv_k = to_col(inv_rows[n_blocks + b:n_blocks + b + 1, :])
            invbuf[pl.ds(b * 128, 128), :] = jnp.where(lane < 64, inv_q, inv_k)

        def head(h, carry):
            cs = pl.ds(pl.multiple_of(h * HEAD_DIM, HEAD_DIM), HEAD_DIM)
            cos_t, sin_t = cos_ref[...], sin_ref[...]

            def rope(v):
                return v * cos_t + pltpu.roll(v, HEAD_DIM // 2, 1) * sin_t

            inv = invbuf[...]
            qh = rope(acc[0, :, cs] * inv[:, 0:1] * gq[layer:layer + 1, cs]).astype(BF16)
            kbuf[:, cs] = rope(acc[1, :, cs] * inv[:, 64:65] * gk[layer:layer + 1, cs]).astype(BF16)
            qb = min(256, tokens)
            for i in range(tokens // qb):
                end = (i + 1) * qb
                s = lax.dot_general(qh[i * qb:end], kbuf[0:end, cs], (((1,), (1,)), ((), ())),
                                    preferred_element_type=F32) * (HEAD_DIM ** -0.5)
                keep = (lax.broadcasted_iota(jnp.int32, (qb, end), 0) + i * qb
                        >= lax.broadcasted_iota(jnp.int32, (qb, end), 1))
                s = jnp.where(keep, s, -jnp.inf)
                e = jnp.exp(s - jnp.max(s, axis=-1, keepdims=True))
                p = (e / jnp.sum(e, axis=-1, keepdims=True)).astype(BF16)
                obuf[i * qb:end, cs] = jnp.dot(p, vbuf[0:end, cs], preferred_element_type=F32).astype(BF16)
            return carry

        with jax.named_scope('heads_%d' % layer):
            lax.fori_loop(0, local_heads, head, 0)
        ck = pltpu.make_async_copy(kbuf, k_out.at[layer], io_sem.at[0])
        cv = pltpu.make_async_copy(vbuf, v_out.at[layer], io_sem.at[1])
        ck.start()
        cv.start()
        return ck, cv

    def out_stage(layer):
        unit = ('o', layer)
        wide_fetch(unit, wb_o, 0, 0)
        wide_stage(unit, obuf, own_rows, wb_o, 0, 2)
        co = scatter_begin(0)
        wide_stage(unit, obuf, own_rows, wb_o, 2, 4)
        with jax.named_scope('sum_o%d' % layer):
            scatter_next(0, co)
            co[2].wait_recv()
            add(0, fin1, eighth, [r2.at[0]], fin.at[0])
            co[3].wait_recv()
            add(0, fin2, eighth, [r2.at[1]], fin.at[1])
        drain(co)
        with jax.named_scope('norm_o%d' % layer):
            add_norm(2 * layer, 3 * layer + 1)

    def mlp_stage(layer):
        cs = [spread_first(4, own_rows, 0), spread_first(4, own_rows, 1)]
        ex = []
        for k, start in ((16, fin1), (17, fin2)):
            ex.append(send(k, hid.at[own_rows, cols(start, eighth)], hid.at[pair_rows, cols(start, eighth)],
                           {'fsdp': pair}))
        service(('u', layer))
        with jax.named_scope('spread_h%d' % layer):
            spread_next(4, own_rows, cs)
        with jax.named_scope('pair_h%d' % layer):
            ex[0].wait_recv()
            ch = [spread_first(12, pair_rows, 0)]
            ex[1].wait_recv()
            ch.append(spread_first(12, pair_rows, 1))
        service(('d', layer))
        finish(('g', layer))
        finish(('u', layer))
        gu_fetch(layer, 0, gu_tile, 0)
        with jax.named_scope('spread_h_last%d' % layer):
            cs[2].wait_recv()
            cs[3].wait_recv()
        cut = gu_whole // 2
        with jax.named_scope('gu_own%d' % layer):
            gu_tiles(layer, own_rows, 0, cut)
        with jax.named_scope('pair_h_next%d' % layer):
            spread_next(12, pair_rows, ch)
        with jax.named_scope('gu_own%d' % layer):
            gu_tiles(layer, own_rows, cut, gu_whole)
        gu_fetch(layer, 0, gu_tile, 0)
        with jax.named_scope('pair_h_last%d' % layer):
            ch[2].wait_recv()
            ch[3].wait_recv()
        with jax.named_scope('gu_pair%d' % layer):
            gu_tiles(layer, pair_rows, 0, gu_whole)
        drain(ex + cs + ch)

        unit = ('d', layer)
        finish(unit)
        wide_fetch(unit, wb_d, 0, 0)
        all_rows = pl.ds(0, 2 * tokens)
        wide_stage(unit, act, all_rows, wb_d, 0, 2)
        cp = scatter_begin(1)
        co = scatter_begin(0)
        wide_stage(unit, act, all_rows, wb_d, 2, 4)
        if layer + 1 < n_layers:
            service(('o', layer + 1))
            service(('q', layer + 1))
        with jax.named_scope('sum_d_next%d' % layer):
            scatter_next(1, cp)
            scatter_next(0, co)
        cp[2].wait_recv()
        add(tokens, fin1, eighth, [r2.at[2]])
        ce = [send(18, part.at[pair_rows, cols(fin1, eighth)], pr.at[0], {'fsdp': pair})]
        cp[3].wait_recv()
        add(tokens, fin2, eighth, [r2.at[3]])
        ce.append(send(19, part.at[pair_rows, cols(fin2, eighth)], pr.at[1], {'fsdp': pair}))
        with jax.named_scope('sum_d_pair%d' % layer):
            co[2].wait_recv()
            ce[0].wait_recv()
            add(0, fin1, eighth, [r2.at[0], pr.at[0]], fin.at[0])
            co[3].wait_recv()
            ce[1].wait_recv()
            add(0, fin2, eighth, [r2.at[1], pr.at[1]], fin.at[1])
        with jax.named_scope('norm_d%d' % layer):
            add_norm(2 * layer + 1, 3 * layer + 2)
        cs = [spread_first(4, own_rows, 0), spread_first(4, own_rows, 1)]
        with jax.named_scope('sum_d_spread%d' % layer):
            spread_next(4, own_rows, cs)
            cs[2].wait_recv()
            cs[3].wait_recv()
        drain(cp + co + ce + cs)

    for d in range(1, n_f):
        rcopy(gains, gbuf.at[f], g_send, g_recv, {'fsdp': lax.rem(f + d, n_f)}).start()
    send_own(0)
    send_own(1)
    load_x = pltpu.make_async_copy(x_in, hid.at[own_rows], io_sem.at[2])
    load_x.start()
    gbuf[f] = gains[...]
    load_x.wait()
    wait_bytes(gbuf.at[pl.ds(0, n_f - 1)], g_recv)
    wait_bytes(gbuf.at[pl.ds(0, n_f - 1)], g_send)
    service(('q', 0))
    service(('o', 0))

    for layer in range(n_layers):
        finish(('q', layer))
        qkv_stage(layer)
        ck, cv = attention_stage(layer)
        service(('g', layer))
        finish(('o', layer))
        out_stage(layer)
        ck.wait()
        cv.wait()
        mlp_stage(layer)

    store_y = pltpu.make_async_copy(hid.at[own_rows], y_out, io_sem.at[2])
    store_y.start()
    for u in range(n_units):
        wait_bytes(units[order[u]][0].at[pl.ds(0, 7)], unit_send.at[u])
    store_y.wait()


def solution(mesh):
    batch_axes = ('dp', 'fsdp')
    act_spec = P(batch_axes, None, None)
    in_cols = P(None, 'fsdp', 'tp')
    in_rows = P(None, 'tp', 'fsdp')
    tp_gain = P(None, 'tp')
    fsdp_gain = P(None, 'fsdp')
    cache_spec = P(None, batch_axes, None, 'tp', None)
    n_f, n_t = mesh.shape['fsdp'], mesh.shape['tp']

    def local_layers(x, w_query, w_key, w_value, w_out, w_gate, w_up, w_down, q_norm_w, k_norm_w, attn_norm_w, ffn_norm_w):
        batch, seq_len, width = x.shape
        n_layers, shard, hw = w_query.shape
        ff = w_gate.shape[2]
        tokens = batch * seq_len
        gains = jnp.stack([attn_norm_w, ffn_norm_w], axis=1).reshape(2 * n_layers, shard)
        gain_rows = -(-2 * n_layers // 8) * 8
        gains = jnp.pad(gains, ((0, gain_rows - 2 * n_layers), (0, 0)))
        cos_t, sin_t = rope_tables(seq_len)
        hbm = pl.BlockSpec(memory_space=pl.ANY)
        vmem = pl.BlockSpec(memory_space=pltpu.VMEM)
        w_gate, w_up = w_gate.transpose(0, 2, 1), w_up.transpose(0, 2, 1)
        ff_half = ff // 2
        layer_bufs = [jax.ShapeDtypeStruct((n_f, 3, shard, hw), BF16), jax.ShapeDtypeStruct((n_f, 1, hw, shard), BF16),
                      jax.ShapeDtypeStruct((n_f, 1, ff_half, shard), BF16),
                      jax.ShapeDtypeStruct((n_f, 1, ff_half, shard), BF16),
                      jax.ShapeDtypeStruct((n_f, 1, ff_half, shard), BF16)]
        out_shape = [jax.ShapeDtypeStruct((tokens, width), BF16), jax.ShapeDtypeStruct((n_layers, tokens, hw), BF16),
                     jax.ShapeDtypeStruct((n_layers, tokens, hw), BF16)] + layer_bufs * n_layers
        sq_rows = -(-2 * (tokens // 128) // 8) * 8
        scratch = [
            pltpu.VMEM((2 * tokens, width), BF16),
            pltpu.VMEM((2, tokens, hw), F32),
            pltpu.VMEM((tokens, hw), BF16),
            pltpu.VMEM((tokens, hw), BF16),
            pltpu.VMEM((tokens, hw), BF16),
            pltpu.VMEM((2 * tokens, ff_half), BF16),
            pltpu.VMEM((2 * tokens, width), BF16),
            pltpu.VMEM((2, tokens, width // 8), BF16),
            pltpu.VMEM((4, tokens, width // 4), BF16),
            pltpu.VMEM((4, tokens, width // 8), BF16),
            pltpu.VMEM((2, tokens, width // 8), BF16),
            pltpu.VMEM((3 * n_layers, n_t, sq_rows, 128), F32),
            pltpu.VMEM((tokens, 128), F32),
            pltpu.VMEM((n_f, gain_rows, shard), F32),
            pltpu.VMEM((2, width, min(256, hw)), BF16),
            pltpu.VMEM((2, 2, min(256, ff_half), width), BF16),
            pltpu.VMEM((2, 2, hw, shard), BF16),
            pltpu.VMEM((2, 2, ff_half, shard), BF16),
            pltpu.SemaphoreType.DMA((5 * n_layers, 8)),
            pltpu.SemaphoreType.DMA((5 * n_layers,)),
            pltpu.SemaphoreType.DMA((2,)),
            pltpu.SemaphoreType.DMA((20,)),
            pltpu.SemaphoreType.DMA((20,)),
            pltpu.SemaphoreType.DMA((3 * n_layers, n_t - 1)),
            pltpu.SemaphoreType.DMA((3 * n_layers, n_t - 1)),
            pltpu.SemaphoreType.DMA,
            pltpu.SemaphoreType.DMA,
            pltpu.SemaphoreType.DMA((3,)),
        ]
        outs = pl.pallas_call(
            lambda *refs: layers_kernel(n_f, n_t, n_layers, *refs),
            name='layers',
            out_shape=out_shape,
            in_specs=[hbm] * 8 + [vmem] * 5,
            out_specs=[hbm] * len(out_shape),
            scratch_shapes=scratch,
            compiler_params=pltpu.CompilerParams(collective_id=0, has_side_effects=True, vmem_limit_bytes=66 * 1000 * 1000),
        )(x.reshape(tokens, width), w_query, w_key, w_value, w_out, w_gate, w_up, w_down,
          q_norm_w, k_norm_w, gains, cos_t, sin_t)
        cache_shape = (n_layers, batch, seq_len, hw // HEAD_DIM, HEAD_DIM)
        return outs[0].reshape(batch, seq_len, width), outs[1].reshape(cache_shape), outs[2].reshape(cache_shape)

    return jax.shard_map(local_layers, mesh=mesh,
                         in_specs=(act_spec, in_cols, in_cols, in_cols, in_rows, in_cols, in_cols, in_rows,
                                   tp_gain, tp_gain, fsdp_gain, fsdp_gain),
                         out_specs=(act_spec, cache_spec, cache_spec), check_vma=False)
```

```python
import jax
import jax.numpy as jnp
from jax import lax
from jax.experimental import pallas as pl
from jax.experimental.pallas import tpu as pltpu
from jax.sharding import PartitionSpec as P

HEAD_DIM = 128
NORM_EPS = 1e-6
ROPE_THETA = 500000.0
MESH = pl.DeviceIdType.MESH
BF16 = jnp.bfloat16
F32 = jnp.float32


def rope_tables(seq_len):
    half = HEAD_DIM // 2
    inv_freq = ROPE_THETA ** (-2.0 * jnp.arange(half, dtype=F32) / HEAD_DIM)
    angles = jnp.arange(seq_len, dtype=F32)[:, None] * inv_freq[None, :]
    cos_t, sin_t = jnp.cos(angles), jnp.sin(angles)
    return jnp.concatenate([cos_t, cos_t], axis=-1), jnp.concatenate([-sin_t, sin_t], axis=-1)


def layers_kernel(n_f, n_t, n_layers, *refs):
    (x_in, wq, wk, wv, wo, wg, wu, wd, gq, gk, gains, cos_ref, sin_ref) = refs[:13]
    y_out, k_out, v_out = refs[13:16]
    bufs = refs[16:16 + 5 * n_layers]
    (hid, acc, kbuf, vbuf, obuf, act, part, fin, r1, r2, pr, sqbuf, invbuf, gbuf,
     wb_qkv, wb_gu, wb_o, wb_d,
     unit_recv, unit_send, ld_sem, ex_recv, ex_send, sq_recv, sq_send, g_recv, g_send, io_sem) = refs[16 + 5 * n_layers:]

    f = lax.axis_index('fsdp')
    t = lax.axis_index('tp')
    tokens, width = x_in.shape
    blk = width // n_f
    hw = kbuf.shape[1]
    local_heads = hw // HEAD_DIM
    ff_half = act.shape[1]
    own_rows, pair_rows = pl.ds(0, tokens), pl.ds(tokens, tokens)

    chip = f // 2
    core = lax.rem(f, 2)
    last_chip = n_f // 2 - 1
    mate = f + 1 - 2 * core
    near = f + 2 - 4 * lax.rem(chip, 2)
    pair = (last_chip - chip) * 2 + core
    near_pair = (last_chip - near // 2) * 2 + core
    cls = chip // 2
    t_a = t + 1 - 2 * lax.rem(t, 2)
    t_b = n_t - 1 - t
    key_a = lax.rem((t + 1) // 2, 2)
    key_b = t // 2

    barrier = pltpu.get_barrier_semaphore()
    for d in range(1, n_f):
        pl.semaphore_signal(barrier, inc=1, device_id={'fsdp': lax.rem(f + d, n_f)}, device_id_type=MESH)
    for d in range(1, n_t):
        pl.semaphore_signal(barrier, inc=1, device_id={'tp': lax.rem(t + d, n_t)}, device_id_type=MESH)
    pl.semaphore_wait(barrier, n_f + n_t - 2)

    def rcopy(src, dst, send_sem, recv_sem, dev):
        return pltpu.make_async_remote_copy(src_ref=src, dst_ref=dst, send_sem=send_sem, recv_sem=recv_sem,
                                            device_id=dev, device_id_type=MESH)

    def half_rows(which):
        return pl.ds(pl.multiple_of(which * ff_half, 16), ff_half)

    units = {}
    order = []
    for layer in range(n_layers):
        b = bufs[5 * layer:5 * layer + 5]
        units['q', layer] = (b[0], [wq.at[layer], wk.at[layer], wv.at[layer]], None)
        units['o', layer] = (b[1], [wo.at[layer]], None)
        units['g', layer] = (b[2], [wg.at[layer, half_rows(cls)]], wg.at[layer, half_rows(1 - cls)])
        units['u', layer] = (b[3], [wu.at[layer, half_rows(cls)]], wu.at[layer, half_rows(1 - cls)])
        units['d', layer] = (b[4], [wd.at[layer, half_rows(cls)]], wd.at[layer, half_rows(1 - cls)])
        first = ['q', 'o'] if layer == 0 else ['o', 'q']
        order += [(name, layer) for name in first + ['g', 'u', 'd']]
    n_units = len(order)
    place = {unit: i for i, unit in enumerate(order)}

    def wait_bytes(ref, sem):
        pltpu.make_async_copy(ref, ref, sem).wait()

    def send_own(unit):
        u = place[unit]
        buf, srcs, other = units[unit]
        for slot, dev in ((1, near), (0, pair), (4, mate)):
            for j, src in enumerate(srcs):
                if slot == 0 and other is not None:
                    src = other
                rcopy(src, buf.at[f, j], unit_send.at[u], unit_recv.at[u, slot], {'fsdp': dev}).start()

    def split(u):
        rows = units[order[u]][0].shape[2]
        if order[u][0] in ('g', 'u', 'd'):
            return rows
        return rows // 2 if order[u][0] == 'q' else rows // 4

    def pass_on(u, src, slot, dev):
        rcopy(src, src, unit_send.at[u], unit_recv.at[u, slot], {'fsdp': dev}).start()

    def service(unit):
        with jax.named_scope('service_%s%d' % unit):
            service_unit(unit)

    def service_unit(unit):
        u = place[unit]
        buf = units[unit][0]
        rows, cut = buf.shape[2], split(u)
        wait_bytes(buf.at[0], unit_recv.at[u, 0])
        pass_on(u, buf.at[pair, :, pl.ds(0, cut)], 2, near)
        pass_on(u, buf.at[pair], 5, mate)
        wait_bytes(buf.at[0], unit_recv.at[u, 1])
        if cut < rows:
            pass_on(u, buf.at[near, :, pl.ds(cut, rows - cut)], 3, pair)
        pass_on(u, buf.at[near], 6, mate)

    def finish(unit):
        with jax.named_scope('finish_%s%d' % unit):
            finish_unit(unit)

    def finish_unit(unit):
        u = place[unit]
        buf = units[unit][0]
        rows, cut = buf.shape[2], split(u)
        wait_bytes(buf.at[0, :, pl.ds(0, cut)], unit_recv.at[u, 2])
        if cut < rows:
            wait_bytes(buf.at[0, :, pl.ds(cut, rows - cut)], unit_recv.at[u, 3])
        pass_on(u, buf.at[near_pair], 7, mate)
        for slot in (4, 5, 6, 7):
            wait_bytes(buf.at[0], unit_recv.at[u, slot])

    def load(unit, j, piece, owner, dst, sem):
        buf, srcs, _ = units[unit]

        @pl.when(owner == f)
        def _():
            pltpu.make_async_copy(srcs[j].at[piece], dst, sem).start()

        @pl.when(owner != f)
        def _():
            pltpu.make_async_copy(buf.at[(owner, j) + piece], dst, sem).start()

    def lanes(start, size):
        return pl.ds(pl.multiple_of(start, size), size)

    def qkv_stage(layer):
        tile = wb_qkv.shape[2]
        n_tiles = hw // tile

        def fetch(j, n, slot):
            for s in range(n_f):
                load(('q', layer), j, (slice(None), lanes(n * tile, tile)), s,
                     wb_qkv.at[slot, pl.ds(s * blk, blk)], ld_sem.at[slot])

        fetch(0, 0, 0)
        for j in range(3):
            def step(n, carry):
                slot = lax.rem(n + j * n_tiles, 2)
                wait_bytes(wb_qkv.at[slot], ld_sem.at[slot])

                @pl.when(n < n_tiles - 1)
                def _():
                    fetch(j, n + 1, 1 - slot)

                if j < 2:
                    @pl.when(n == n_tiles - 1)
                    def _():
                        fetch(j + 1, 0, 1 - slot)

                val = jnp.dot(hid[own_rows, :], wb_qkv[slot], preferred_element_type=F32)
                if j < 2:
                    acc[j, :, lanes(n * tile, tile)] = val
                else:
                    vbuf[:, lanes(n * tile, tile)] = val.astype(BF16)
                return carry

            with jax.named_scope('qkv%d_%d' % (j, layer)):
                lax.fori_loop(0, n_tiles, step, 0)

    gu_tile = min(256, ff_half)
    gu_whole = ff_half // gu_tile
    gu_rest = ff_half - gu_whole * gu_tile

    def gu_fetch(layer, n, size, slot):
        for j, name in enumerate(('g', 'u')):
            for s in range(n_f):
                start = n * gu_tile
                if not isinstance(start, int):
                    start = pl.multiple_of(start, gu_tile)
                load((name, layer), 0, (pl.ds(start, size),), s,
                     wb_gu.at[slot, j, pl.ds(0, size), pl.ds(s * blk, blk)], ld_sem.at[slot])

    def gu_tile_product(size, slot, rs, out_cols):
        lhs = hid[rs, :]
        dims = (((1,), (1,)), ((), ()))
        g = lax.dot_general(lhs, wb_gu[slot, 0, 0:size, :], dims, preferred_element_type=F32)
        up = lax.dot_general(lhs, wb_gu[slot, 1, 0:size, :], dims, preferred_element_type=F32)
        act[rs, out_cols] = (g / (1.0 + jnp.exp(-g)) * up).astype(BF16)

    def gu_tiles(layer, rs, lo, hi):
        def step(n, carry):
            slot = lax.rem(n, 2)
            wait_bytes(wb_gu.at[slot], ld_sem.at[slot])

            @pl.when(n < gu_whole - 1)
            def _():
                gu_fetch(layer, n + 1, gu_tile, 1 - slot)

            if gu_rest and hi == gu_whole:
                @pl.when(n == gu_whole - 1)
                def _():
                    gu_fetch(layer, gu_whole, gu_rest, 1 - slot)

            gu_tile_product(gu_tile, slot, rs, lanes(n * gu_tile, gu_tile))
            return carry

        lax.fori_loop(lo, hi, step, 0)
        if gu_rest and hi == gu_whole:
            slot = gu_whole % 2
            wait_bytes(wb_gu.at[slot, :, pl.ds(0, gu_rest)], ld_sem.at[slot])
            gu_tile_product(gu_rest, slot, rs, pl.ds(gu_whole * gu_tile, gu_rest))

    def wide_segment(g):
        side, kept = lax.rem(g, 2), g // 2
        key = key_a + (key_b - key_a) * side
        return 2 * side + key * kept + (1 - key) * (1 - kept)

    def wide_fetch(unit, wb, g, slot):
        for e in range(2):
            load(unit, 0, (), 2 * wide_segment(g) + e, wb.at[slot, e], ld_sem.at[slot])

    def wide_stage(unit, lhs, out_rows, wb, lo, hi):
        def step(g, carry):
            slot = lax.rem(g, 2)
            wait_bytes(wb.at[slot], ld_sem.at[slot])

            @pl.when(g < 3)
            def _():
                wide_fetch(unit, wb, g + 1, 1 - slot)

            for e in range(2):
                val = jnp.dot(lhs[...], wb[slot, e], preferred_element_type=F32)
                start = (2 * wide_segment(g) + e) * blk
                part[out_rows, pl.ds(pl.multiple_of(start, blk), blk)] = val.astype(BF16)
            return carry

        with jax.named_scope('wide_%s%d' % unit):
            lax.fori_loop(lo, hi, step, 0)

    rows = min(128, tokens)

    def by_rows(body, total=tokens):
        def step(i, carry):
            body(i * rows)
            return carry

        lax.fori_loop(0, total // rows, step, 0)

    def chunk(start):
        return pl.ds(pl.multiple_of(start, rows), rows)

    quarter, eighth, half = width // 4, width // 8, width // 2
    keep1, keep2 = key_a * quarter, half + key_b * quarter
    fin1, fin2 = keep1 + key_b * eighth, keep2 + key_a * eighth

    def cols(start, size):
        return pl.ds(pl.multiple_of(start, eighth), size)

    def send(k, src, dst, dev):
        copy = rcopy(src, dst, ex_send.at[k], ex_recv.at[k], dev)
        copy.start()
        return copy

    def add(row0, start, size, others, dst=None):
        def body(r):
            val = part[chunk(row0 + r), cols(start, size)].astype(F32)
            for other in others:
                val = val + other[chunk(r), :].astype(F32)
            if dst is None:
                part[chunk(row0 + r), cols(start, size)] = val.astype(BF16)
            else:
                dst[chunk(r), :] = val.astype(BF16)

        by_rows(body)

    def scatter_begin(g):
        rs = pl.ds(g * tokens, tokens)
        return [send(8 * g, part.at[rs, cols((1 - key_a) * quarter, quarter)], r1.at[2 * g], {'tp': t_a}),
                send(8 * g + 1, part.at[rs, cols(half + (1 - key_b) * quarter, quarter)], r1.at[2 * g + 1], {'tp': t_b})]

    def scatter_next(g, cs):
        rs, row0 = pl.ds(g * tokens, tokens), g * tokens
        cs[0].wait_recv()
        add(row0, keep1, quarter, [r1.at[2 * g]])
        cs.append(send(8 * g + 2, part.at[rs, cols(keep1 + (1 - key_b) * eighth, eighth)], r2.at[2 * g], {'tp': t_b}))
        cs[1].wait_recv()
        add(row0, keep2, quarter, [r1.at[2 * g + 1]])
        cs.append(send(8 * g + 3, part.at[rs, cols(keep2 + (1 - key_a) * eighth, eighth)], r2.at[2 * g + 1], {'tp': t_a}))

    def spread_first(k, rs, which):
        start, dev = ((fin1, t_b), (fin2, t_a))[which]
        view = hid.at[rs, cols(start, eighth)]
        return send(k + which, view, view, {'tp': dev})

    def spread_next(k, rs, cs):
        cs[0].wait_recv()
        view = hid.at[rs, cols(keep1, quarter)]
        cs.append(send(k + 2, view, view, {'tp': t_a}))
        cs[1].wait_recv()
        view = hid.at[rs, cols(keep2, quarter)]
        cs.append(send(k + 3, view, view, {'tp': t_b}))

    def drain(cs):
        for c in cs:
            c.wait_send()

    n_blocks = tokens // 128
    lane = lax.broadcasted_iota(jnp.int32, (128, 128), 1)
    eye = lax.broadcasted_iota(jnp.int32, (128, 128), 0) == lane

    def to_row(col):
        return jnp.sum(jnp.where(eye, col, 0.0), axis=0, keepdims=True)

    def to_col(row):
        return jnp.sum(jnp.where(eye, row, 0.0), axis=1, keepdims=True)

    def inverse_rms(k):
        copies = []
        for d in range(1, n_t):
            c = rcopy(sqbuf.at[k, 0], sqbuf.at[k, d], sq_send.at[k, d - 1], sq_recv.at[k, d - 1],
                      {'tp': lax.rem(t + d, n_t)})
            c.start()
            copies.append(c)
        with jax.named_scope('squares_%d' % k):
            for c in copies:
                c.wait_recv()
            drain(copies)
        tot = sqbuf[k, 0]
        for d in range(1, n_t):
            tot = tot + sqbuf[k, d]
        return lax.rsqrt(tot / width + NORM_EPS)

    def add_norm(row, k):
        for b in range(n_blocks):
            rs = pl.ds(b * 128, 128)
            a0, a1 = fin[0, rs, :].astype(F32), fin[1, rs, :].astype(F32)
            col = jnp.sum(a0 * a0, axis=-1, keepdims=True) + jnp.sum(a1 * a1, axis=-1, keepdims=True)
            sqbuf[k, 0, b:b + 1, :] = to_row(col)
        inv = inverse_rms(k)
        for b in range(n_blocks):
            rs = pl.ds(b * 128, 128)
            scale = to_col(inv[b:b + 1, :])
            for e, start in ((0, fin1), (1, fin2)):
                gain = gbuf[start // eighth, row:row + 1, :]
                hid[rs, cols(start, eighth)] = (hid[rs, cols(start, eighth)].astype(F32)
                                                + fin[e, rs, :].astype(F32) * scale * gain).astype(BF16)

    def attention_stage(layer):
        for which in range(2):
            for b in range(n_blocks):
                vals = acc[which, pl.ds(b * 128, 128), :]
                row = which * n_blocks + b
                sqbuf[3 * layer, 0, row:row + 1, :] = to_row(jnp.sum(vals * vals, axis=-1, keepdims=True))
        inv_rows = inverse_rms(3 * layer)
        for b in range(n_blocks):
            inv_q = to_col(inv_rows[b:b + 1, :])
            inv_k = to_col(inv_rows[n_blocks + b:n_blocks + b + 1, :])
            invbuf[pl.ds(b * 128, 128), :] = jnp.where(lane < 64, inv_q, inv_k)

        def head(h, carry):
            cs = pl.ds(pl.multiple_of(h * HEAD_DIM, HEAD_DIM), HEAD_DIM)
            cos_t, sin_t = cos_ref[...], sin_ref[...]

            def rope(v):
                return v * cos_t + pltpu.roll(v, HEAD_DIM // 2, 1) * sin_t

            inv = invbuf[...]
            qh = rope(acc[0, :, cs] * inv[:, 0:1] * gq[layer:layer + 1, cs]).astype(BF16)
            kbuf[:, cs] = rope(acc[1, :, cs] * inv[:, 64:65] * gk[layer:layer + 1, cs]).astype(BF16)
            qb = min(256, tokens)
            for i in range(tokens // qb):
                end = (i + 1) * qb
                s = lax.dot_general(qh[i * qb:end], kbuf[0:end, cs], (((1,), (1,)), ((), ())),
                                    preferred_element_type=F32) * (HEAD_DIM ** -0.5)
                keep = (lax.broadcasted_iota(jnp.int32, (qb, end), 0) + i * qb
                        >= lax.broadcasted_iota(jnp.int32, (qb, end), 1))
                s = jnp.where(keep, s, -jnp.inf)
                e = jnp.exp(s - jnp.max(s, axis=-1, keepdims=True))
                p = (e / jnp.sum(e, axis=-1, keepdims=True)).astype(BF16)
                obuf[i * qb:end, cs] = jnp.dot(p, vbuf[0:end, cs], preferred_element_type=F32).astype(BF16)
            return carry

        with jax.named_scope('heads_%d' % layer):
            lax.fori_loop(0, local_heads, head, 0)
        ck = pltpu.make_async_copy(kbuf, k_out.at[layer], io_sem.at[0])
        cv = pltpu.make_async_copy(vbuf, v_out.at[layer], io_sem.at[1])
        ck.start()
        cv.start()
        return ck, cv

    def out_stage(layer):
        unit = ('o', layer)
        wide_fetch(unit, wb_o, 0, 0)
        wide_stage(unit, obuf, own_rows, wb_o, 0, 2)
        co = scatter_begin(0)
        wide_stage(unit, obuf, own_rows, wb_o, 2, 4)
        with jax.named_scope('sum_o%d' % layer):
            scatter_next(0, co)
            if layer == 0:
                service(('g', 0))
            else:
                service(('u', layer))
                send_own(('d', layer))
            co[2].wait_recv()
            add(0, fin1, eighth, [r2.at[0]], fin.at[0])
            co[3].wait_recv()
            add(0, fin2, eighth, [r2.at[1]], fin.at[1])
        drain(co)
        with jax.named_scope('norm_o%d' % layer):
            add_norm(2 * layer, 3 * layer + 1)

    def mlp_stage(layer):
        cs = [spread_first(4, own_rows, 0), spread_first(4, own_rows, 1)]
        ex = []
        for k, start in ((16, fin1), (17, fin2)):
            ex.append(send(k, hid.at[own_rows, cols(start, eighth)], hid.at[pair_rows, cols(start, eighth)],
                           {'fsdp': pair}))
        if layer == 0:
            service(('u', 0))
            send_own(('d', 0))
        with jax.named_scope('spread_h%d' % layer):
            spread_next(4, own_rows, cs)
        with jax.named_scope('pair_h%d' % layer):
            ex[0].wait_recv()
            ch = [spread_first(12, pair_rows, 0)]
            ex[1].wait_recv()
            ch.append(spread_first(12, pair_rows, 1))
        finish(('g', layer))
        finish(('u', layer))
        gu_fetch(layer, 0, gu_tile, 0)
        with jax.named_scope('spread_h_last%d' % layer):
            cs[2].wait_recv()
            cs[3].wait_recv()
        cut = gu_whole // 2
        with jax.named_scope('gu_own%d' % layer):
            gu_tiles(layer, own_rows, 0, cut)
        with jax.named_scope('pair_h_next%d' % layer):
            spread_next(12, pair_rows, ch)
        if layer > 0:
            service(('d', layer))
        with jax.named_scope('gu_own%d' % layer):
            gu_tiles(layer, own_rows, cut, gu_whole)
        gu_fetch(layer, 0, gu_tile, 0)
        with jax.named_scope('pair_h_last%d' % layer):
            ch[2].wait_recv()
            ch[3].wait_recv()
        if layer == 0:
            service(('d', 0))
        if layer + 1 < n_layers:
            send_own(('o', layer + 1))
            send_own(('q', layer + 1))
        with jax.named_scope('gu_pair%d' % layer):
            gu_tiles(layer, pair_rows, 0, gu_whole)
        drain(ex + cs + ch)

        unit = ('d', layer)
        finish(unit)
        wide_fetch(unit, wb_d, 0, 0)
        all_rows = pl.ds(0, 2 * tokens)
        wide_stage(unit, act, all_rows, wb_d, 0, 2)
        cp = scatter_begin(1)
        wide_stage(unit, act, all_rows, wb_d, 2, 4)
        with jax.named_scope('sum_d_pair%d' % layer):
            scatter_next(1, cp)
            co = scatter_begin(0)
            cp[2].wait_recv()
            add(tokens, fin1, eighth, [r2.at[2]])
            ce = [send(18, part.at[pair_rows, cols(fin1, eighth)], pr.at[0], {'fsdp': pair})]
            cp[3].wait_recv()
            add(tokens, fin2, eighth, [r2.at[3]])
            ce.append(send(19, part.at[pair_rows, cols(fin2, eighth)], pr.at[1], {'fsdp': pair}))
        with jax.named_scope('sum_d_next%d' % layer):
            scatter_next(0, co)
        with jax.named_scope('sum_d_last%d' % layer):
            co[2].wait_recv()
            ce[0].wait_recv()
            add(0, fin1, eighth, [r2.at[0], pr.at[0]], fin.at[0])
            co[3].wait_recv()
            ce[1].wait_recv()
            add(0, fin2, eighth, [r2.at[1], pr.at[1]], fin.at[1])
        with jax.named_scope('norm_d%d' % layer):
            add_norm(2 * layer + 1, 3 * layer + 2)
        cs = [spread_first(4, own_rows, 0), spread_first(4, own_rows, 1)]
        if layer + 1 < n_layers:
            service(('o', layer + 1))
            service(('q', layer + 1))
            send_own(('g', layer + 1))
            send_own(('u', layer + 1))
        with jax.named_scope('sum_d_spread%d' % layer):
            spread_next(4, own_rows, cs)
            cs[2].wait_recv()
            cs[3].wait_recv()
        drain(cp + co + ce + cs)

    for d in range(1, n_f):
        rcopy(gains, gbuf.at[f], g_send, g_recv, {'fsdp': lax.rem(f + d, n_f)}).start()
    send_own(('q', 0))
    load_x = pltpu.make_async_copy(x_in, hid.at[own_rows], io_sem.at[2])
    load_x.start()
    gbuf[f] = gains[...]
    load_x.wait()
    wait_bytes(gbuf.at[pl.ds(0, n_f - 1)], g_recv)
    wait_bytes(gbuf.at[pl.ds(0, n_f - 1)], g_send)
    service(('q', 0))
    send_own(('o', 0))

    for layer in range(n_layers):
        finish(('q', layer))
        qkv_stage(layer)
        if layer == 0:
            service(('o', 0))
            send_own(('g', 0))
            send_own(('u', 0))
        else:
            service(('g', layer))
        ck, cv = attention_stage(layer)
        finish(('o', layer))
        out_stage(layer)
        ck.wait()
        cv.wait()
        mlp_stage(layer)

    store_y = pltpu.make_async_copy(hid.at[own_rows], y_out, io_sem.at[2])
    store_y.start()
    for u in range(n_units):
        wait_bytes(units[order[u]][0].at[pl.ds(0, 7)], unit_send.at[u])
    store_y.wait()


def solution(mesh):
    batch_axes = ('dp', 'fsdp')
    act_spec = P(batch_axes, None, None)
    in_cols = P(None, 'fsdp', 'tp')
    in_rows = P(None, 'tp', 'fsdp')
    tp_gain = P(None, 'tp')
    fsdp_gain = P(None, 'fsdp')
    cache_spec = P(None, batch_axes, None, 'tp', None)
    n_f, n_t = mesh.shape['fsdp'], mesh.shape['tp']

    def local_layers(x, w_query, w_key, w_value, w_out, w_gate, w_up, w_down, q_norm_w, k_norm_w, attn_norm_w, ffn_norm_w):
        batch, seq_len, width = x.shape
        n_layers, shard, hw = w_query.shape
        ff = w_gate.shape[2]
        tokens = batch * seq_len
        gains = jnp.stack([attn_norm_w, ffn_norm_w], axis=1).reshape(2 * n_layers, shard)
        gain_rows = -(-2 * n_layers // 8) * 8
        gains = jnp.pad(gains, ((0, gain_rows - 2 * n_layers), (0, 0)))
        cos_t, sin_t = rope_tables(seq_len)
        hbm = pl.BlockSpec(memory_space=pl.ANY)
        vmem = pl.BlockSpec(memory_space=pltpu.VMEM)
        w_gate, w_up = w_gate.transpose(0, 2, 1), w_up.transpose(0, 2, 1)
        ff_half = ff // 2
        layer_bufs = [jax.ShapeDtypeStruct((n_f, 3, shard, hw), BF16), jax.ShapeDtypeStruct((n_f, 1, hw, shard), BF16),
                      jax.ShapeDtypeStruct((n_f, 1, ff_half, shard), BF16),
                      jax.ShapeDtypeStruct((n_f, 1, ff_half, shard), BF16),
                      jax.ShapeDtypeStruct((n_f, 1, ff_half, shard), BF16)]
        out_shape = [jax.ShapeDtypeStruct((tokens, width), BF16), jax.ShapeDtypeStruct((n_layers, tokens, hw), BF16),
                     jax.ShapeDtypeStruct((n_layers, tokens, hw), BF16)] + layer_bufs * n_layers
        sq_rows = -(-2 * (tokens // 128) // 8) * 8
        scratch = [
            pltpu.VMEM((2 * tokens, width), BF16),
            pltpu.VMEM((2, tokens, hw), F32),
            pltpu.VMEM((tokens, hw), BF16),
            pltpu.VMEM((tokens, hw), BF16),
            pltpu.VMEM((tokens, hw), BF16),
            pltpu.VMEM((2 * tokens, ff_half), BF16),
            pltpu.VMEM((2 * tokens, width), BF16),
            pltpu.VMEM((2, tokens, width // 8), BF16),
            pltpu.VMEM((4, tokens, width // 4), BF16),
            pltpu.VMEM((4, tokens, width // 8), BF16),
            pltpu.VMEM((2, tokens, width // 8), BF16),
            pltpu.VMEM((3 * n_layers, n_t, sq_rows, 128), F32),
            pltpu.VMEM((tokens, 128), F32),
            pltpu.VMEM((n_f, gain_rows, shard), F32),
            pltpu.VMEM((2, width, min(256, hw)), BF16),
            pltpu.VMEM((2, 2, min(256, ff_half), width), BF16),
            pltpu.VMEM((2, 2, hw, shard), BF16),
            pltpu.VMEM((2, 2, ff_half, shard), BF16),
            pltpu.SemaphoreType.DMA((5 * n_layers, 8)),
            pltpu.SemaphoreType.DMA((5 * n_layers,)),
            pltpu.SemaphoreType.DMA((2,)),
            pltpu.SemaphoreType.DMA((20,)),
            pltpu.SemaphoreType.DMA((20,)),
            pltpu.SemaphoreType.DMA((3 * n_layers, n_t - 1)),
            pltpu.SemaphoreType.DMA((3 * n_layers, n_t - 1)),
            pltpu.SemaphoreType.DMA,
            pltpu.SemaphoreType.DMA,
            pltpu.SemaphoreType.DMA((3,)),
        ]
        outs = pl.pallas_call(
            lambda *refs: layers_kernel(n_f, n_t, n_layers, *refs),
            name='layers',
            out_shape=out_shape,
            in_specs=[hbm] * 8 + [vmem] * 5,
            out_specs=[hbm] * len(out_shape),
            scratch_shapes=scratch,
            compiler_params=pltpu.CompilerParams(collective_id=0, has_side_effects=True, vmem_limit_bytes=66 * 1000 * 1000),
        )(x.reshape(tokens, width), w_query, w_key, w_value, w_out, w_gate, w_up, w_down,
          q_norm_w, k_norm_w, gains, cos_t, sin_t)
        cache_shape = (n_layers, batch, seq_len, hw // HEAD_DIM, HEAD_DIM)
        return outs[0].reshape(batch, seq_len, width), outs[1].reshape(cache_shape), outs[2].reshape(cache_shape)

    return jax.shard_map(local_layers, mesh=mesh,
                         in_specs=(act_spec, in_cols, in_cols, in_cols, in_rows, in_cols, in_cols, in_rows,
                                   tp_gain, tp_gain, fsdp_gain, fsdp_gain),
                         out_specs=(act_spec, cache_spec, cache_spec), check_vma=False)
```

```python
import jax
import jax.numpy as jnp
from jax import lax
from jax.experimental import pallas as pl
from jax.experimental.pallas import tpu as pltpu
from jax.sharding import PartitionSpec as P

HEAD_DIM = 128
NORM_EPS = 1e-6
ROPE_THETA = 500000.0
MESH = pl.DeviceIdType.MESH
BF16 = jnp.bfloat16
F32 = jnp.float32


def rope_tables(seq_len):
    half = HEAD_DIM // 2
    inv_freq = ROPE_THETA ** (-2.0 * jnp.arange(half, dtype=F32) / HEAD_DIM)
    angles = jnp.arange(seq_len, dtype=F32)[:, None] * inv_freq[None, :]
    cos_t, sin_t = jnp.cos(angles), jnp.sin(angles)
    return jnp.concatenate([cos_t, cos_t], axis=-1), jnp.concatenate([-sin_t, sin_t], axis=-1)


def layers_kernel(n_f, n_t, n_layers, *refs):
    (x_in, wq, wk, wv, wo, wg, wu, wd, gq, gk, gains, cos_ref, sin_ref) = refs[:13]
    y_out, k_out, v_out = refs[13:16]
    bufs = refs[16:16 + 5 * n_layers]
    (hid, acc, kbuf, vbuf, obuf, act, part, fin, r1, r2, pr, sqbuf, invbuf, gbuf,
     wb_qkv, wb_gu, wb_o, wb_d,
     unit_recv, unit_send, ld_sem, ex_recv, ex_send, sq_recv, sq_send, g_recv, g_send, io_sem) = refs[16 + 5 * n_layers:]

    f = lax.axis_index('fsdp')
    t = lax.axis_index('tp')
    tokens, width = x_in.shape
    blk = width // n_f
    hw = kbuf.shape[1]
    local_heads = hw // HEAD_DIM
    ff_half = act.shape[1]
    own_rows, pair_rows = pl.ds(0, tokens), pl.ds(tokens, tokens)

    chip = f // 2
    core = lax.rem(f, 2)
    last_chip = n_f // 2 - 1
    mate = f + 1 - 2 * core
    near = f + 2 - 4 * lax.rem(chip, 2)
    pair = (last_chip - chip) * 2 + core
    near_pair = (last_chip - near // 2) * 2 + core
    cls = chip // 2
    t_a = t + 1 - 2 * lax.rem(t, 2)
    t_b = n_t - 1 - t
    key_a = lax.rem((t + 1) // 2, 2)
    key_b = t // 2

    barrier = pltpu.get_barrier_semaphore()
    for d in range(1, n_f):
        pl.semaphore_signal(barrier, inc=1, device_id={'fsdp': lax.rem(f + d, n_f)}, device_id_type=MESH)
    for d in range(1, n_t):
        pl.semaphore_signal(barrier, inc=1, device_id={'tp': lax.rem(t + d, n_t)}, device_id_type=MESH)
    pl.semaphore_wait(barrier, n_f + n_t - 2)

    def rcopy(src, dst, send_sem, recv_sem, dev):
        return pltpu.make_async_remote_copy(src_ref=src, dst_ref=dst, send_sem=send_sem, recv_sem=recv_sem,
                                            device_id=dev, device_id_type=MESH)

    def half_rows(which):
        return pl.ds(pl.multiple_of(which * ff_half, 16), ff_half)

    units = {}
    order = []
    for layer in range(n_layers):
        b = bufs[5 * layer:5 * layer + 5]
        units['q', layer] = (b[0], [wq.at[layer], wk.at[layer], wv.at[layer]], None)
        units['o', layer] = (b[1], [wo.at[layer]], None)
        units['g', layer] = (b[2], [wg.at[layer, half_rows(cls)]], wg.at[layer, half_rows(1 - cls)])
        units['u', layer] = (b[3], [wu.at[layer, half_rows(cls)]], wu.at[layer, half_rows(1 - cls)])
        units['d', layer] = (b[4], [wd.at[layer, half_rows(cls)]], wd.at[layer, half_rows(1 - cls)])
        first = ['q', 'o'] if layer == 0 else ['o', 'q']
        order += [(name, layer) for name in first + ['g', 'u', 'd']]
    n_units = len(order)
    place = {unit: i for i, unit in enumerate(order)}

    def wait_bytes(ref, sem):
        pltpu.make_async_copy(ref, ref, sem).wait()

    def send_own(unit):
        u = place[unit]
        buf, srcs, other = units[unit]
        for slot, dev in ((1, near), (0, pair), (4, mate)):
            for j, src in enumerate(srcs):
                if slot == 0 and other is not None:
                    src = other
                rcopy(src, buf.at[f, j], unit_send.at[u], unit_recv.at[u, slot], {'fsdp': dev}).start()

    def split(u):
        rows = units[order[u]][0].shape[2]
        if order[u][0] in ('g', 'u', 'd'):
            return rows
        return rows // 8 * 3 if order[u][0] == 'q' else rows // 4

    def pass_on(u, src, slot, dev):
        rcopy(src, src, unit_send.at[u], unit_recv.at[u, slot], {'fsdp': dev}).start()

    def service(unit):
        with jax.named_scope('service_%s%d' % unit):
            service_unit(unit)

    def service_unit(unit):
        u = place[unit]
        buf = units[unit][0]
        rows, cut = buf.shape[2], split(u)
        wait_bytes(buf.at[0], unit_recv.at[u, 0])
        pass_on(u, buf.at[pair, :, pl.ds(0, cut)], 2, near)
        pass_on(u, buf.at[pair], 5, mate)
        wait_bytes(buf.at[0], unit_recv.at[u, 1])
        if cut < rows:
            pass_on(u, buf.at[near, :, pl.ds(cut, rows - cut)], 3, pair)
        pass_on(u, buf.at[near], 6, mate)

    def finish(unit):
        with jax.named_scope('finish_%s%d' % unit):
            finish_far(unit)
            finish_near(unit)

    def finish_near(unit):
        for slot in (4, 5, 6):
            wait_bytes(units[unit][0].at[0], unit_recv.at[place[unit], slot])

    def finish_far(unit):
        u = place[unit]
        buf = units[unit][0]
        rows, cut = buf.shape[2], split(u)
        wait_bytes(buf.at[0, :, pl.ds(0, cut)], unit_recv.at[u, 2])
        if cut < rows:
            wait_bytes(buf.at[0, :, pl.ds(cut, rows - cut)], unit_recv.at[u, 3])
        pass_on(u, buf.at[near_pair], 7, mate)
        wait_bytes(buf.at[0], unit_recv.at[u, 7])

    rows = min(128, tokens)

    def by_rows(body):
        def step(i, carry):
            body(i * rows)
            return carry

        lax.fori_loop(0, tokens // rows, step, 0)

    def chunk(start):
        return pl.ds(pl.multiple_of(start, rows), rows)

    def load(unit, j, piece, owner, dst, sem):
        buf, srcs, _ = units[unit]

        @pl.when(owner == f)
        def _():
            pltpu.make_async_copy(srcs[j].at[piece], dst, sem).start()

        @pl.when(owner != f)
        def _():
            pltpu.make_async_copy(buf.at[(owner, j) + piece], dst, sem).start()

    def lanes(start, size):
        return pl.ds(pl.multiple_of(start, size), size)

    chips = [chip, near // 2, pair // 2, near_pair // 2]
    by_chip = part.at[own_rows]

    def arrange():
        def body(r):
            for pos, c in enumerate(chips):
                by_chip[chunk(r), pl.ds(pos * 2 * blk, 2 * blk)] = hid[chunk(r), lanes(c * 2 * blk, 2 * blk)]

        by_rows(body)

    def qkv_phase(layer, first, last):
        tile = wb_qkv.shape[2]
        n_tiles = hw // tile
        buf, srcs, _ = units['q', layer]
        depth = (last - first) * 2 * blk

        def fetch(i, slot):
            j, cs = i // n_tiles, lanes(lax.rem(i, n_tiles) * tile, tile)
            for pos in range(first, last):
                for e in range(2):
                    owner = 2 * chips[pos] + e
                    dst = wb_qkv.at[slot, pl.ds((2 * (pos - first) + e) * blk, blk)]

                    def remote():
                        pltpu.make_async_copy(buf.at[owner, j, :, cs], dst, ld_sem.at[slot]).start()

                    if pos > 0:
                        remote()
                        continue
                    pl.when(owner != f)(remote)
                    for jj, src in enumerate(srcs):
                        @pl.when((owner == f) & (j == jj))
                        def _():
                            pltpu.make_async_copy(src.at[:, cs], dst, ld_sem.at[slot]).start()

        def step(i, carry):
            slot = lax.rem(i, 2)
            wait_bytes(wb_qkv.at[slot, pl.ds(0, depth)], ld_sem.at[slot])

            @pl.when(i < 3 * n_tiles - 1)
            def _():
                fetch(i + 1, 1 - slot)

            val = jnp.dot(by_chip[:, pl.ds(first * 2 * blk, depth)], wb_qkv[slot, 0:depth, :],
                          preferred_element_type=F32)
            j, cs = i // n_tiles, lanes(lax.rem(i, n_tiles) * tile, tile)
            if first:
                acc[j, :, cs] += val
            else:
                acc[j, :, cs] = val
            return carry

        fetch(0, 0)
        with jax.named_scope('qkv%d_%d' % (first, layer)):
            lax.fori_loop(0, 3 * n_tiles, step, 0)

    def qkv_stage(layer):
        arrange()
        with jax.named_scope('finish_near%d' % layer):
            finish_near(('q', layer))
        qkv_phase(layer, 0, 3)
        with jax.named_scope('finish_far%d' % layer):
            finish_far(('q', layer))
        qkv_phase(layer, 3, 4)

    gu_tile = min(256, ff_half)
    gu_whole = ff_half // gu_tile
    gu_rest = ff_half - gu_whole * gu_tile

    def gu_fetch(layer, n, size, slot):
        for j, name in enumerate(('g', 'u')):
            for s in range(n_f):
                start = n * gu_tile
                if not isinstance(start, int):
                    start = pl.multiple_of(start, gu_tile)
                load((name, layer), 0, (pl.ds(start, size),), s,
                     wb_gu.at[slot, j, pl.ds(0, size), pl.ds(s * blk, blk)], ld_sem.at[slot])

    def gu_tile_product(size, slot, rs, out_cols):
        lhs = hid[rs, :]
        dims = (((1,), (1,)), ((), ()))
        g = lax.dot_general(lhs, wb_gu[slot, 0, 0:size, :], dims, preferred_element_type=F32)
        up = lax.dot_general(lhs, wb_gu[slot, 1, 0:size, :], dims, preferred_element_type=F32)
        act[rs, out_cols] = (g / (1.0 + jnp.exp(-g)) * up).astype(BF16)

    def gu_tiles(layer, rs, at_tile, action):
        def step(n, carry):
            slot = lax.rem(n, 2)
            if action is not None:
                pl.when(n == at_tile)(action)
            wait_bytes(wb_gu.at[slot], ld_sem.at[slot])

            @pl.when(n < gu_whole - 1)
            def _():
                gu_fetch(layer, n + 1, gu_tile, 1 - slot)

            if gu_rest:
                @pl.when(n == gu_whole - 1)
                def _():
                    gu_fetch(layer, gu_whole, gu_rest, 1 - slot)

            gu_tile_product(gu_tile, slot, rs, lanes(n * gu_tile, gu_tile))
            return carry

        lax.fori_loop(0, gu_whole, step, 0)
        if gu_rest:
            slot = gu_whole % 2
            wait_bytes(wb_gu.at[slot, :, pl.ds(0, gu_rest)], ld_sem.at[slot])
            gu_tile_product(gu_rest, slot, rs, pl.ds(gu_whole * gu_tile, gu_rest))

    def wide_segment(g):
        side, kept = lax.rem(g, 2), g // 2
        key = key_a + (key_b - key_a) * side
        return 2 * side + key * kept + (1 - key) * (1 - kept)

    def wide_fetch(unit, wb, g, slot):
        for e in range(2):
            load(unit, 0, (), 2 * wide_segment(g) + e, wb.at[slot, e], ld_sem.at[slot])

    def wide_stage(unit, lhs, out_rows, wb, lo, hi):
        def step(g, carry):
            slot = lax.rem(g, 2)
            wait_bytes(wb.at[slot], ld_sem.at[slot])

            @pl.when(g < 3)
            def _():
                wide_fetch(unit, wb, g + 1, 1 - slot)

            for e in range(2):
                val = jnp.dot(lhs[...], wb[slot, e], preferred_element_type=F32)
                start = (2 * wide_segment(g) + e) * blk
                part[out_rows, pl.ds(pl.multiple_of(start, blk), blk)] = val.astype(BF16)
            return carry

        with jax.named_scope('wide_%s%d' % unit):
            lax.fori_loop(lo, hi, step, 0)

    quarter, eighth, half = width // 4, width // 8, width // 2
    keep1, keep2 = key_a * quarter, half + key_b * quarter
    fin1, fin2 = keep1 + key_b * eighth, keep2 + key_a * eighth

    def cols(start, size):
        return pl.ds(pl.multiple_of(start, eighth), size)

    def send(k, src, dst, dev):
        copy = rcopy(src, dst, ex_send.at[k], ex_recv.at[k], dev)
        copy.start()
        return copy

    def add(row0, start, size, others, dst=None):
        def body(r):
            val = part[chunk(row0 + r), cols(start, size)].astype(F32)
            for other in others:
                val = val + other[chunk(r), :].astype(F32)
            if dst is None:
                part[chunk(row0 + r), cols(start, size)] = val.astype(BF16)
            else:
                dst[chunk(r), :] = val.astype(BF16)

        by_rows(body)

    def scatter_begin(g):
        rs = pl.ds(g * tokens, tokens)
        return [send(8 * g, part.at[rs, cols((1 - key_a) * quarter, quarter)], r1.at[2 * g], {'tp': t_a}),
                send(8 * g + 1, part.at[rs, cols(half + (1 - key_b) * quarter, quarter)], r1.at[2 * g + 1], {'tp': t_b})]

    def scatter_next(g, cs):
        rs, row0 = pl.ds(g * tokens, tokens), g * tokens
        cs[0].wait_recv()
        add(row0, keep1, quarter, [r1.at[2 * g]])
        cs.append(send(8 * g + 2, part.at[rs, cols(keep1 + (1 - key_b) * eighth, eighth)], r2.at[2 * g], {'tp': t_b}))
        cs[1].wait_recv()
        add(row0, keep2, quarter, [r1.at[2 * g + 1]])
        cs.append(send(8 * g + 3, part.at[rs, cols(keep2 + (1 - key_a) * eighth, eighth)], r2.at[2 * g + 1], {'tp': t_a}))

    def spread_copy(k, rs, i):
        start, size, dev = ((fin1, eighth, t_b), (fin2, eighth, t_a), (keep1, quarter, t_a), (keep2, quarter, t_b))[i]
        view = hid.at[rs, cols(start, size)]
        return rcopy(view, view, ex_send.at[k + i], ex_recv.at[k + i], {'tp': dev})

    def spread_first(k, rs, which):
        copy = spread_copy(k, rs, which)
        copy.start()
        return copy

    def spread_next(k, rs, cs):
        for i in (2, 3):
            cs[i - 2].wait_recv()
            cs.append(spread_copy(k, rs, i))
            cs[i].start()

    def drain(cs):
        for c in cs:
            c.wait_send()

    n_blocks = tokens // 128
    lane = lax.broadcasted_iota(jnp.int32, (128, 128), 1)
    eye = lax.broadcasted_iota(jnp.int32, (128, 128), 0) == lane

    def to_row(col):
        return jnp.sum(jnp.where(eye, col, 0.0), axis=0, keepdims=True)

    def to_col(row):
        return jnp.sum(jnp.where(eye, row, 0.0), axis=1, keepdims=True)

    def inverse_rms(k):
        copies = []
        for d in range(1, n_t):
            c = rcopy(sqbuf.at[k, 0], sqbuf.at[k, d], sq_send.at[k, d - 1], sq_recv.at[k, d - 1],
                      {'tp': lax.rem(t + d, n_t)})
            c.start()
            copies.append(c)
        with jax.named_scope('squares_%d' % k):
            for c in copies:
                c.wait_recv()
            drain(copies)
        tot = sqbuf[k, 0]
        for d in range(1, n_t):
            tot = tot + sqbuf[k, d]
        return lax.rsqrt(tot / width + NORM_EPS)

    def add_norm(row, k):
        for b in range(n_blocks):
            rs = pl.ds(b * 128, 128)
            a0, a1 = fin[0, rs, :].astype(F32), fin[1, rs, :].astype(F32)
            col = jnp.sum(a0 * a0, axis=-1, keepdims=True) + jnp.sum(a1 * a1, axis=-1, keepdims=True)
            sqbuf[k, 0, b:b + 1, :] = to_row(col)
        inv = inverse_rms(k)
        for b in range(n_blocks):
            rs = pl.ds(b * 128, 128)
            scale = to_col(inv[b:b + 1, :])
            for e, start in ((0, fin1), (1, fin2)):
                gain = gbuf[start // eighth, row:row + 1, :]
                hid[rs, cols(start, eighth)] = (hid[rs, cols(start, eighth)].astype(F32)
                                                + fin[e, rs, :].astype(F32) * scale * gain).astype(BF16)

    def attention_stage(layer):
        for which in range(2):
            for b in range(n_blocks):
                vals = acc[which, pl.ds(b * 128, 128), :]
                row = which * n_blocks + b
                sqbuf[3 * layer, 0, row:row + 1, :] = to_row(jnp.sum(vals * vals, axis=-1, keepdims=True))
        inv_rows = inverse_rms(3 * layer)
        for b in range(n_blocks):
            inv_q = to_col(inv_rows[b:b + 1, :])
            inv_k = to_col(inv_rows[n_blocks + b:n_blocks + b + 1, :])
            invbuf[pl.ds(b * 128, 128), :] = jnp.where(lane < 64, inv_q, inv_k)

        def head(h, carry):
            cs = pl.ds(pl.multiple_of(h * HEAD_DIM, HEAD_DIM), HEAD_DIM)
            cos_t, sin_t = cos_ref[...], sin_ref[...]

            def rope(v):
                return v * cos_t + pltpu.roll(v, HEAD_DIM // 2, 1) * sin_t

            inv = invbuf[...]
            qh = rope(acc[0, :, cs] * inv[:, 0:1] * gq[layer:layer + 1, cs]).astype(BF16)
            kbuf[:, cs] = rope(acc[1, :, cs] * inv[:, 64:65] * gk[layer:layer + 1, cs]).astype(BF16)
            vbuf[:, cs] = acc[2, :, cs].astype(BF16)
            qb = min(256, tokens)
            for i in range(tokens // qb):
                end = (i + 1) * qb
                s = lax.dot_general(qh[i * qb:end], kbuf[0:end, cs], (((1,), (1,)), ((), ())),
                                    preferred_element_type=F32) * (HEAD_DIM ** -0.5)
                keep = (lax.broadcasted_iota(jnp.int32, (qb, end), 0) + i * qb
                        >= lax.broadcasted_iota(jnp.int32, (qb, end), 1))
                s = jnp.where(keep, s, -jnp.inf)
                e = jnp.exp(s - jnp.max(s, axis=-1, keepdims=True))
                p = (e / jnp.sum(e, axis=-1, keepdims=True)).astype(BF16)
                obuf[i * qb:end, cs] = jnp.dot(p, vbuf[0:end, cs], preferred_element_type=F32).astype(BF16)
            return carry

        with jax.named_scope('heads_%d' % layer):
            lax.fori_loop(0, local_heads, head, 0)
        ck = pltpu.make_async_copy(kbuf, k_out.at[layer], io_sem.at[0])
        cv = pltpu.make_async_copy(vbuf, v_out.at[layer], io_sem.at[1])
        ck.start()
        cv.start()
        return ck, cv

    def out_stage(layer):
        unit = ('o', layer)
        wide_fetch(unit, wb_o, 0, 0)
        wide_stage(unit, obuf, own_rows, wb_o, 0, 2)
        co = scatter_begin(0)
        wide_stage(unit, obuf, own_rows, wb_o, 2, 4)
        with jax.named_scope('sum_o%d' % layer):
            scatter_next(0, co)
            if layer == 0:
                service(('g', 0))
            else:
                service(('u', layer))
                send_own(('d', layer))
            co[2].wait_recv()
            add(0, fin1, eighth, [r2.at[0]], fin.at[0])
            co[3].wait_recv()
            add(0, fin2, eighth, [r2.at[1]], fin.at[1])
        drain(co)
        with jax.named_scope('norm_o%d' % layer):
            add_norm(2 * layer, 3 * layer + 1)

    def mlp_stage(layer):
        cs = [spread_first(4, own_rows, 0), spread_first(4, own_rows, 1)]
        ex = []
        for k, start in ((16, fin1), (17, fin2)):
            ex.append(send(k, hid.at[own_rows, cols(start, eighth)], hid.at[pair_rows, cols(start, eighth)],
                           {'fsdp': pair}))
        if layer == 0:
            service(('u', 0))
            send_own(('d', 0))
        with jax.named_scope('spread_h%d' % layer):
            spread_next(4, own_rows, cs)
        with jax.named_scope('pair_h%d' % layer):
            ex[0].wait_recv()
            ch = [spread_first(12, pair_rows, 0)]
            ex[1].wait_recv()
            ch.append(spread_first(12, pair_rows, 1))
        finish(('g', layer))
        finish(('u', layer))
        gu_fetch(layer, 0, gu_tile, 0)
        with jax.named_scope('spread_h_last%d' % layer):
            cs[2].wait_recv()
            cs[3].wait_recv()

        def pair_next():
            ch[0].wait_recv()
            spread_copy(12, pair_rows, 2).start()
            ch[1].wait_recv()
            spread_copy(12, pair_rows, 3).start()
            if layer > 0:
                service(('d', layer))

        with jax.named_scope('gu_own%d' % layer):
            gu_tiles(layer, own_rows, gu_whole // 2, pair_next)
        gu_fetch(layer, 0, gu_tile, 0)
        with jax.named_scope('pair_h_last%d' % layer):
            for i in (2, 3):
                ch.append(spread_copy(12, pair_rows, i))
                ch[i].wait_recv()
        if layer == 0:
            service(('d', 0))
        if layer + 1 < n_layers:
            send_own(('o', layer + 1))
            send_own(('q', layer + 1))
        with jax.named_scope('gu_pair%d' % layer):
            gu_tiles(layer, pair_rows, 0, None)
        drain(ex + cs + ch)

        unit = ('d', layer)
        finish(unit)
        wide_fetch(unit, wb_d, 0, 0)
        all_rows = pl.ds(0, 2 * tokens)
        wide_stage(unit, act, all_rows, wb_d, 0, 2)
        cp = scatter_begin(1)
        wide_stage(unit, act, all_rows, wb_d, 2, 4)
        with jax.named_scope('sum_d_pair%d' % layer):
            scatter_next(1, cp)
            co = scatter_begin(0)
            cp[2].wait_recv()
            add(tokens, fin1, eighth, [r2.at[2]])
            ce = [send(18, part.at[pair_rows, cols(fin1, eighth)], pr.at[0], {'fsdp': pair})]
            cp[3].wait_recv()
            add(tokens, fin2, eighth, [r2.at[3]])
            ce.append(send(19, part.at[pair_rows, cols(fin2, eighth)], pr.at[1], {'fsdp': pair}))
        with jax.named_scope('sum_d_next%d' % layer):
            scatter_next(0, co)
        with jax.named_scope('sum_d_last%d' % layer):
            co[2].wait_recv()
            ce[0].wait_recv()
            add(0, fin1, eighth, [r2.at[0], pr.at[0]], fin.at[0])
            co[3].wait_recv()
            ce[1].wait_recv()
            add(0, fin2, eighth, [r2.at[1], pr.at[1]], fin.at[1])
        with jax.named_scope('norm_d%d' % layer):
            add_norm(2 * layer + 1, 3 * layer + 2)
        cs = [spread_first(4, own_rows, 0), spread_first(4, own_rows, 1)]
        if layer + 1 < n_layers:
            service(('o', layer + 1))
            service(('q', layer + 1))
            send_own(('g', layer + 1))
            send_own(('u', layer + 1))
        with jax.named_scope('sum_d_spread%d' % layer):
            spread_next(4, own_rows, cs)
            cs[2].wait_recv()
            cs[3].wait_recv()
        drain(cp + co + ce + cs)

    for d in range(1, n_f):
        rcopy(gains, gbuf.at[f], g_send, g_recv, {'fsdp': lax.rem(f + d, n_f)}).start()
    send_own(('q', 0))
    load_x = pltpu.make_async_copy(x_in, hid.at[own_rows], io_sem.at[2])
    load_x.start()
    gbuf[f] = gains[...]
    load_x.wait()
    wait_bytes(gbuf.at[pl.ds(0, n_f - 1)], g_recv)
    wait_bytes(gbuf.at[pl.ds(0, n_f - 1)], g_send)
    service(('q', 0))
    send_own(('o', 0))

    for layer in range(n_layers):
        qkv_stage(layer)
        if layer == 0:
            service(('o', 0))
            send_own(('g', 0))
            send_own(('u', 0))
        else:
            service(('g', layer))
        ck, cv = attention_stage(layer)
        finish(('o', layer))
        out_stage(layer)
        ck.wait()
        cv.wait()
        mlp_stage(layer)

    store_y = pltpu.make_async_copy(hid.at[own_rows], y_out, io_sem.at[2])
    store_y.start()
    for u in range(n_units):
        wait_bytes(units[order[u]][0].at[pl.ds(0, 7)], unit_send.at[u])
    store_y.wait()


def solution(mesh):
    batch_axes = ('dp', 'fsdp')
    act_spec = P(batch_axes, None, None)
    in_cols = P(None, 'fsdp', 'tp')
    in_rows = P(None, 'tp', 'fsdp')
    tp_gain = P(None, 'tp')
    fsdp_gain = P(None, 'fsdp')
    cache_spec = P(None, batch_axes, None, 'tp', None)
    n_f, n_t = mesh.shape['fsdp'], mesh.shape['tp']

    def local_layers(x, w_query, w_key, w_value, w_out, w_gate, w_up, w_down, q_norm_w, k_norm_w, attn_norm_w, ffn_norm_w):
        batch, seq_len, width = x.shape
        n_layers, shard, hw = w_query.shape
        ff = w_gate.shape[2]
        tokens = batch * seq_len
        gains = jnp.stack([attn_norm_w, ffn_norm_w], axis=1).reshape(2 * n_layers, shard)
        gain_rows = -(-2 * n_layers // 8) * 8
        gains = jnp.pad(gains, ((0, gain_rows - 2 * n_layers), (0, 0)))
        cos_t, sin_t = rope_tables(seq_len)
        hbm = pl.BlockSpec(memory_space=pl.ANY)
        vmem = pl.BlockSpec(memory_space=pltpu.VMEM)
        w_gate, w_up = w_gate.transpose(0, 2, 1), w_up.transpose(0, 2, 1)
        ff_half = ff // 2
        layer_bufs = [jax.ShapeDtypeStruct((n_f, 3, shard, hw), BF16), jax.ShapeDtypeStruct((n_f, 1, hw, shard), BF16),
                      jax.ShapeDtypeStruct((n_f, 1, ff_half, shard), BF16),
                      jax.ShapeDtypeStruct((n_f, 1, ff_half, shard), BF16),
                      jax.ShapeDtypeStruct((n_f, 1, ff_half, shard), BF16)]
        out_shape = [jax.ShapeDtypeStruct((tokens, width), BF16), jax.ShapeDtypeStruct((n_layers, tokens, hw), BF16),
                     jax.ShapeDtypeStruct((n_layers, tokens, hw), BF16)] + layer_bufs * n_layers
        sq_rows = -(-2 * (tokens // 128) // 8) * 8
        scratch = [
            pltpu.VMEM((2 * tokens, width), BF16),
            pltpu.VMEM((3, tokens, hw), F32),
            pltpu.VMEM((tokens, hw), BF16),
            pltpu.VMEM((tokens, hw), BF16),
            pltpu.VMEM((tokens, hw), BF16),
            pltpu.VMEM((2 * tokens, ff_half), BF16),
            pltpu.VMEM((2 * tokens, width), BF16),
            pltpu.VMEM((2, tokens, width // 8), BF16),
            pltpu.VMEM((4, tokens, width // 4), BF16),
            pltpu.VMEM((4, tokens, width // 8), BF16),
            pltpu.VMEM((2, tokens, width // 8), BF16),
            pltpu.VMEM((3 * n_layers, n_t, sq_rows, 128), F32),
            pltpu.VMEM((tokens, 128), F32),
            pltpu.VMEM((n_f, gain_rows, shard), F32),
            pltpu.VMEM((2, 6 * shard, min(256, hw)), BF16),
            pltpu.VMEM((2, 2, min(256, ff_half), width), BF16),
            pltpu.VMEM((2, 2, hw, shard), BF16),
            pltpu.VMEM((2, 2, ff_half, shard), BF16),
            pltpu.SemaphoreType.DMA((5 * n_layers, 8)),
            pltpu.SemaphoreType.DMA((5 * n_layers,)),
            pltpu.SemaphoreType.DMA((2,)),
            pltpu.SemaphoreType.DMA((20,)),
            pltpu.SemaphoreType.DMA((20,)),
            pltpu.SemaphoreType.DMA((3 * n_layers, n_t - 1)),
            pltpu.SemaphoreType.DMA((3 * n_layers, n_t - 1)),
            pltpu.SemaphoreType.DMA,
            pltpu.SemaphoreType.DMA,
            pltpu.SemaphoreType.DMA((3,)),
        ]
        outs = pl.pallas_call(
            lambda *refs: layers_kernel(n_f, n_t, n_layers, *refs),
            name='layers',
            out_shape=out_shape,
            in_specs=[hbm] * 8 + [vmem] * 5,
            out_specs=[hbm] * len(out_shape),
            scratch_shapes=scratch,
            compiler_params=pltpu.CompilerParams(collective_id=0, has_side_effects=True, vmem_limit_bytes=66 * 1000 * 1000),
        )(x.reshape(tokens, width), w_query, w_key, w_value, w_out, w_gate, w_up, w_down,
          q_norm_w, k_norm_w, gains, cos_t, sin_t)
        cache_shape = (n_layers, batch, seq_len, hw // HEAD_DIM, HEAD_DIM)
        return outs[0].reshape(batch, seq_len, width), outs[1].reshape(cache_shape), outs[2].reshape(cache_shape)

    return jax.shard_map(local_layers, mesh=mesh,
                         in_specs=(act_spec, in_cols, in_cols, in_cols, in_rows, in_cols, in_cols, in_rows,
                                   tp_gain, tp_gain, fsdp_gain, fsdp_gain),
                         out_specs=(act_spec, cache_spec, cache_spec), check_vma=False)
```

```python
import jax
import jax.numpy as jnp
from jax import lax
from jax.experimental import pallas as pl
from jax.experimental.pallas import tpu as pltpu
from jax.sharding import PartitionSpec as P

HEAD_DIM = 128
NORM_EPS = 1e-6
ROPE_THETA = 500000.0
MESH = pl.DeviceIdType.MESH
BF16 = jnp.bfloat16
F32 = jnp.float32


def rope_tables(seq_len):
    half = HEAD_DIM // 2
    inv_freq = ROPE_THETA ** (-2.0 * jnp.arange(half, dtype=F32) / HEAD_DIM)
    angles = jnp.arange(seq_len, dtype=F32)[:, None] * inv_freq[None, :]
    cos_t, sin_t = jnp.cos(angles), jnp.sin(angles)
    return jnp.concatenate([cos_t, cos_t], axis=-1), jnp.concatenate([-sin_t, sin_t], axis=-1)


def layers_kernel(n_f, n_t, n_layers, *refs):
    (x_in, wq, wk, wv, wo, wg, wu, wd, gq, gk, gains, cos_ref, sin_ref) = refs[:13]
    y_out, k_out, v_out = refs[13:16]
    bufs = refs[16:16 + 5 * n_layers]
    (hid, acc, kbuf, vbuf, obuf, act, part, fin, r1, r2, pr, sqbuf, invbuf, gbuf,
     wb_qkv, wb_gu, wb_o, wb_d,
     unit_recv, unit_send, ld_sem, ex_recv, ex_send, sq_recv, sq_send, g_recv, g_send, io_sem) = refs[16 + 5 * n_layers:]

    f = lax.axis_index('fsdp')
    t = lax.axis_index('tp')
    tokens, width = x_in.shape
    blk = width // n_f
    hw = kbuf.shape[1]
    local_heads = hw // HEAD_DIM
    ff_half = act.shape[1]
    own_rows, pair_rows = pl.ds(0, tokens), pl.ds(tokens, tokens)

    chip = f // 2
    core = lax.rem(f, 2)
    last_chip = n_f // 2 - 1
    mate = f + 1 - 2 * core
    near = f + 2 - 4 * lax.rem(chip, 2)
    pair = (last_chip - chip) * 2 + core
    near_pair = (last_chip - near // 2) * 2 + core
    cls = chip // 2
    t_a = t + 1 - 2 * lax.rem(t, 2)
    t_b = n_t - 1 - t
    key_a = lax.rem((t + 1) // 2, 2)
    key_b = t // 2

    barrier = pltpu.get_barrier_semaphore()
    for d in range(1, n_f):
        pl.semaphore_signal(barrier, inc=1, device_id={'fsdp': lax.rem(f + d, n_f)}, device_id_type=MESH)
    for d in range(1, n_t):
        pl.semaphore_signal(barrier, inc=1, device_id={'tp': lax.rem(t + d, n_t)}, device_id_type=MESH)
    pl.semaphore_wait(barrier, n_f + n_t - 2)

    def rcopy(src, dst, send_sem, recv_sem, dev):
        return pltpu.make_async_remote_copy(src_ref=src, dst_ref=dst, send_sem=send_sem, recv_sem=recv_sem,
                                            device_id=dev, device_id_type=MESH)

    def half_rows(which):
        return pl.ds(pl.multiple_of(which * ff_half, 16), ff_half)

    units = {}
    order = []
    for layer in range(n_layers):
        b = bufs[5 * layer:5 * layer + 5]
        units['q', layer] = (b[0], [wq.at[layer], wk.at[layer], wv.at[layer]], None)
        units['o', layer] = (b[1], [wo.at[layer]], None)
        units['g', layer] = (b[2], [wg.at[layer, half_rows(cls)]], wg.at[layer, half_rows(1 - cls)])
        units['u', layer] = (b[3], [wu.at[layer, half_rows(cls)]], wu.at[layer, half_rows(1 - cls)])
        units['d', layer] = (b[4], [wd.at[layer, half_rows(cls)]], wd.at[layer, half_rows(1 - cls)])
        first = ['q', 'o'] if layer == 0 else ['o', 'q']
        order += [(name, layer) for name in first + ['g', 'u', 'd']]
    n_units = len(order)
    place = {unit: i for i, unit in enumerate(order)}

    def wait_bytes(ref, sem):
        pltpu.make_async_copy(ref, ref, sem).wait()

    def send_own(unit):
        u = place[unit]
        buf, srcs, other = units[unit]
        for slot, dev in ((1, near), (0, pair), (4, mate)):
            for j, src in enumerate(srcs):
                if slot == 0 and other is not None:
                    src = other
                rcopy(src, buf.at[f, j], unit_send.at[u], unit_recv.at[u, slot], {'fsdp': dev}).start()

    def split(u):
        rows = units[order[u]][0].shape[2]
        if order[u][0] in ('g', 'u', 'd'):
            return rows
        return rows // 2 if order[u][0] == 'q' else rows // 4

    def pass_on(u, src, slot, dev):
        rcopy(src, src, unit_send.at[u], unit_recv.at[u, slot], {'fsdp': dev}).start()

    def service(unit):
        with jax.named_scope('service_%s%d' % unit):
            service_unit(unit)

    def service_unit(unit):
        u = place[unit]
        buf = units[unit][0]
        rows, cut = buf.shape[2], split(u)
        wait_bytes(buf.at[0], unit_recv.at[u, 0])
        pass_on(u, buf.at[pair, :, pl.ds(0, cut)], 2, near)
        pass_on(u, buf.at[pair], 5, mate)
        wait_bytes(buf.at[0], unit_recv.at[u, 1])
        if cut < rows:
            pass_on(u, buf.at[near, :, pl.ds(cut, rows - cut)], 3, pair)
        pass_on(u, buf.at[near], 6, mate)

    def finish(unit):
        with jax.named_scope('finish_%s%d' % unit):
            finish_far(unit)
            finish_near(unit)

    def finish_near(unit):
        for slot in (4, 5, 6):
            wait_bytes(units[unit][0].at[0], unit_recv.at[place[unit], slot])

    def finish_far(unit):
        u = place[unit]
        buf = units[unit][0]
        rows, cut = buf.shape[2], split(u)
        wait_bytes(buf.at[0, :, pl.ds(0, cut)], unit_recv.at[u, 2])
        if cut < rows:
            wait_bytes(buf.at[0, :, pl.ds(cut, rows - cut)], unit_recv.at[u, 3])
        pass_on(u, buf.at[near_pair], 7, mate)
        wait_bytes(buf.at[0], unit_recv.at[u, 7])

    rows = min(128, tokens)

    def by_rows(body):
        def step(i, carry):
            body(i * rows)
            return carry

        lax.fori_loop(0, tokens // rows, step, 0)

    def chunk(start):
        return pl.ds(pl.multiple_of(start, rows), rows)

    def load(unit, j, piece, owner, dst, sem):
        buf, srcs, _ = units[unit]

        @pl.when(owner == f)
        def _():
            pltpu.make_async_copy(srcs[j].at[piece], dst, sem).start()

        @pl.when(owner != f)
        def _():
            pltpu.make_async_copy(buf.at[(owner, j) + piece], dst, sem).start()

    def lanes(start, size):
        return pl.ds(pl.multiple_of(start, size), size)

    chips = [chip, near // 2, pair // 2, near_pair // 2]
    by_chip = part.at[own_rows]

    def arrange():
        def body(r):
            for pos, c in enumerate(chips):
                by_chip[chunk(r), pl.ds(pos * 2 * blk, 2 * blk)] = hid[chunk(r), lanes(c * 2 * blk, 2 * blk)]

        by_rows(body)

    def qkv_phase(layer, first, last):
        tile = wb_o.shape[3] if first else wb_qkv.shape[2]
        n_tiles = hw // tile
        buf, srcs, _ = units['q', layer]

        def slots(slot):
            return wb_o.at[slot, 0] if first else wb_qkv.at[slot]

        depth = (last - first) * 2 * blk

        def fetch(i, slot):
            j, cs = i // n_tiles, lanes(lax.rem(i, n_tiles) * tile, tile)
            for pos in range(first, last):
                for e in range(2):
                    owner = 2 * chips[pos] + e
                    dst = slots(slot).at[pl.ds((2 * (pos - first) + e) * blk, blk)]

                    def remote():
                        pltpu.make_async_copy(buf.at[owner, j, :, cs], dst, ld_sem.at[slot]).start()

                    if pos > 0:
                        remote()
                        continue
                    pl.when(owner != f)(remote)
                    for jj, src in enumerate(srcs):
                        @pl.when((owner == f) & (j == jj))
                        def _():
                            pltpu.make_async_copy(src.at[:, cs], dst, ld_sem.at[slot]).start()

        def step(i, carry):
            slot = lax.rem(i, 2)
            wait_bytes(slots(slot).at[pl.ds(0, depth)], ld_sem.at[slot])

            @pl.when(i < 3 * n_tiles - 1)
            def _():
                fetch(i + 1, 1 - slot)

            val = jnp.dot(by_chip[:, pl.ds(first * 2 * blk, depth)], slots(slot)[0:depth, :],
                          preferred_element_type=F32)
            j, cs = i // n_tiles, lanes(lax.rem(i, n_tiles) * tile, tile)
            if first:
                acc[j, :, cs] += val
            else:
                acc[j, :, cs] = val
            return carry

        fetch(0, 0)
        with jax.named_scope('qkv%d_%d' % (first, layer)):
            lax.fori_loop(0, 3 * n_tiles, step, 0)

    def qkv_stage(layer):
        arrange()
        with jax.named_scope('finish_near%d' % layer):
            finish_near(('q', layer))
        qkv_phase(layer, 0, 3)
        with jax.named_scope('finish_far%d' % layer):
            finish_far(('q', layer))
        qkv_phase(layer, 3, 4)

    gu_tile = min(256, ff_half)
    gu_whole = ff_half // gu_tile
    gu_rest = ff_half - gu_whole * gu_tile

    def gu_fetch(layer, n, size, slot):
        for j, name in enumerate(('g', 'u')):
            for s in range(n_f):
                start = n * gu_tile
                if not isinstance(start, int):
                    start = pl.multiple_of(start, gu_tile)
                load((name, layer), 0, (pl.ds(start, size),), s,
                     wb_gu.at[slot, j, pl.ds(0, size), pl.ds(s * blk, blk)], ld_sem.at[slot])

    def gu_tile_product(size, slot, rs, out_cols):
        lhs = hid[rs, :]
        dims = (((1,), (1,)), ((), ()))
        g = lax.dot_general(lhs, wb_gu[slot, 0, 0:size, :], dims, preferred_element_type=F32)
        up = lax.dot_general(lhs, wb_gu[slot, 1, 0:size, :], dims, preferred_element_type=F32)
        act[rs, out_cols] = (g / (1.0 + jnp.exp(-g)) * up).astype(BF16)

    def gu_tiles(layer, rs, at_tile, action):
        def step(n, carry):
            slot = lax.rem(n, 2)
            if action is not None:
                pl.when(n == at_tile)(action)
            wait_bytes(wb_gu.at[slot], ld_sem.at[slot])

            @pl.when(n < gu_whole - 1)
            def _():
                gu_fetch(layer, n + 1, gu_tile, 1 - slot)

            if gu_rest:
                @pl.when(n == gu_whole - 1)
                def _():
                    gu_fetch(layer, gu_whole, gu_rest, 1 - slot)

            gu_tile_product(gu_tile, slot, rs, lanes(n * gu_tile, gu_tile))
            return carry

        lax.fori_loop(0, gu_whole, step, 0)
        if gu_rest:
            slot = gu_whole % 2
            wait_bytes(wb_gu.at[slot, :, pl.ds(0, gu_rest)], ld_sem.at[slot])
            gu_tile_product(gu_rest, slot, rs, pl.ds(gu_whole * gu_tile, gu_rest))

    def wide_segment(g):
        side, kept = lax.rem(g, 2), g // 2
        key = key_a + (key_b - key_a) * side
        return 2 * side + key * kept + (1 - key) * (1 - kept)

    def wide_fetch(unit, wb, g, slot):
        for e in range(2):
            load(unit, 0, (), 2 * wide_segment(g) + e, wb.at[slot, e], ld_sem.at[slot])

    def wide_stage(unit, lhs, out_rows, wb, lo, hi):
        def step(g, carry):
            slot = lax.rem(g, 2)
            wait_bytes(wb.at[slot], ld_sem.at[slot])

            @pl.when(g < 3)
            def _():
                wide_fetch(unit, wb, g + 1, 1 - slot)

            for e in range(2):
                val = jnp.dot(lhs[...], wb[slot, e], preferred_element_type=F32)
                start = (2 * wide_segment(g) + e) * blk
                part[out_rows, pl.ds(pl.multiple_of(start, blk), blk)] = val.astype(BF16)
            return carry

        with jax.named_scope('wide_%s%d' % unit):
            lax.fori_loop(lo, hi, step, 0)

    quarter, eighth, half = width // 4, width // 8, width // 2
    keep1, keep2 = key_a * quarter, half + key_b * quarter
    fin1, fin2 = keep1 + key_b * eighth, keep2 + key_a * eighth

    def cols(start, size):
        return pl.ds(pl.multiple_of(start, eighth), size)

    def send(k, src, dst, dev):
        copy = rcopy(src, dst, ex_send.at[k], ex_recv.at[k], dev)
        copy.start()
        return copy

    def add(row0, start, size, others, dst=None):
        def body(r):
            val = part[chunk(row0 + r), cols(start, size)].astype(F32)
            for other in others:
                val = val + other[chunk(r), :].astype(F32)
            if dst is None:
                part[chunk(row0 + r), cols(start, size)] = val.astype(BF16)
            else:
                dst[chunk(r), :] = val.astype(BF16)

        by_rows(body)

    def scatter_begin(g):
        rs = pl.ds(g * tokens, tokens)
        return [send(8 * g, part.at[rs, cols((1 - key_a) * quarter, quarter)], r1.at[2 * g], {'tp': t_a}),
                send(8 * g + 1, part.at[rs, cols(half + (1 - key_b) * quarter, quarter)], r1.at[2 * g + 1], {'tp': t_b})]

    def scatter_next(g, cs):
        rs, row0 = pl.ds(g * tokens, tokens), g * tokens
        cs[0].wait_recv()
        add(row0, keep1, quarter, [r1.at[2 * g]])
        cs.append(send(8 * g + 2, part.at[rs, cols(keep1 + (1 - key_b) * eighth, eighth)], r2.at[2 * g], {'tp': t_b}))
        cs[1].wait_recv()
        add(row0, keep2, quarter, [r1.at[2 * g + 1]])
        cs.append(send(8 * g + 3, part.at[rs, cols(keep2 + (1 - key_a) * eighth, eighth)], r2.at[2 * g + 1], {'tp': t_a}))

    def spread_copy(k, rs, i):
        start, size, dev = ((fin1, eighth, t_b), (fin2, eighth, t_a), (keep1, quarter, t_a), (keep2, quarter, t_b))[i]
        view = hid.at[rs, cols(start, size)]
        return rcopy(view, view, ex_send.at[k + i], ex_recv.at[k + i], {'tp': dev})

    def spread_first(k, rs, which):
        copy = spread_copy(k, rs, which)
        copy.start()
        return copy

    def spread_next(k, rs, cs):
        for i in (2, 3):
            cs[i - 2].wait_recv()
            cs.append(spread_copy(k, rs, i))
            cs[i].start()

    def drain(cs):
        for c in cs:
            c.wait_send()

    n_blocks = tokens // 128
    lane = lax.broadcasted_iota(jnp.int32, (128, 128), 1)
    eye = lax.broadcasted_iota(jnp.int32, (128, 128), 0) == lane

    def to_row(col):
        return jnp.sum(jnp.where(eye, col, 0.0), axis=0, keepdims=True)

    def to_col(row):
        return jnp.sum(jnp.where(eye, row, 0.0), axis=1, keepdims=True)

    def inverse_rms(k):
        copies = []
        for d in range(1, n_t):
            c = rcopy(sqbuf.at[k, 0], sqbuf.at[k, d], sq_send.at[k, d - 1], sq_recv.at[k, d - 1],
                      {'tp': lax.rem(t + d, n_t)})
            c.start()
            copies.append(c)
        with jax.named_scope('squares_%d' % k):
            for c in copies:
                c.wait_recv()
            drain(copies)
        tot = sqbuf[k, 0]
        for d in range(1, n_t):
            tot = tot + sqbuf[k, d]
        return lax.rsqrt(tot / width + NORM_EPS)

    def add_norm(row, k):
        for b in range(n_blocks):
            rs = pl.ds(b * 128, 128)
            a0, a1 = fin[0, rs, :].astype(F32), fin[1, rs, :].astype(F32)
            col = jnp.sum(a0 * a0, axis=-1, keepdims=True) + jnp.sum(a1 * a1, axis=-1, keepdims=True)
            sqbuf[k, 0, b:b + 1, :] = to_row(col)
        inv = inverse_rms(k)
        for b in range(n_blocks):
            rs = pl.ds(b * 128, 128)
            scale = to_col(inv[b:b + 1, :])
            for e, start in ((0, fin1), (1, fin2)):
                gain = gbuf[start // eighth, row:row + 1, :]
                hid[rs, cols(start, eighth)] = (hid[rs, cols(start, eighth)].astype(F32)
                                                + fin[e, rs, :].astype(F32) * scale * gain).astype(BF16)

    def attention_stage(layer):
        for which in range(2):
            for b in range(n_blocks):
                vals = acc[which, pl.ds(b * 128, 128), :]
                row = which * n_blocks + b
                sqbuf[3 * layer, 0, row:row + 1, :] = to_row(jnp.sum(vals * vals, axis=-1, keepdims=True))
        inv_rows = inverse_rms(3 * layer)
        if layer == 0:
            service(('o', 0))
            send_own(('g', 0))
            send_own(('u', 0))
        for b in range(n_blocks):
            inv_q = to_col(inv_rows[b:b + 1, :])
            inv_k = to_col(inv_rows[n_blocks + b:n_blocks + b + 1, :])
            invbuf[pl.ds(b * 128, 128), :] = jnp.where(lane < 64, inv_q, inv_k)

        def head(h, carry):
            cs = pl.ds(pl.multiple_of(h * HEAD_DIM, HEAD_DIM), HEAD_DIM)
            cos_t, sin_t = cos_ref[...], sin_ref[...]

            def rope(v):
                return v * cos_t + pltpu.roll(v, HEAD_DIM // 2, 1) * sin_t

            inv = invbuf[...]
            qh = rope(acc[0, :, cs] * inv[:, 0:1] * gq[layer:layer + 1, cs]).astype(BF16)
            kbuf[:, cs] = rope(acc[1, :, cs] * inv[:, 64:65] * gk[layer:layer + 1, cs]).astype(BF16)
            vbuf[:, cs] = acc[2, :, cs].astype(BF16)
            qb = min(256, tokens)
            for i in range(tokens // qb):
                end = (i + 1) * qb
                s = lax.dot_general(qh[i * qb:end], kbuf[0:end, cs], (((1,), (1,)), ((), ())),
                                    preferred_element_type=F32) * (HEAD_DIM ** -0.5)
                keep = (lax.broadcasted_iota(jnp.int32, (qb, end), 0) + i * qb
                        >= lax.broadcasted_iota(jnp.int32, (qb, end), 1))
                s = jnp.where(keep, s, -jnp.inf)
                e = jnp.exp(s - jnp.max(s, axis=-1, keepdims=True))
                p = (e / jnp.sum(e, axis=-1, keepdims=True)).astype(BF16)
                obuf[i * qb:end, cs] = jnp.dot(p, vbuf[0:end, cs], preferred_element_type=F32).astype(BF16)
            return carry

        with jax.named_scope('heads_%d' % layer):
            lax.fori_loop(0, local_heads, head, 0)
        ck = pltpu.make_async_copy(kbuf, k_out.at[layer], io_sem.at[0])
        cv = pltpu.make_async_copy(vbuf, v_out.at[layer], io_sem.at[1])
        ck.start()
        cv.start()
        return ck, cv

    def out_stage(layer):
        unit = ('o', layer)
        wide_fetch(unit, wb_o, 0, 0)
        wide_stage(unit, obuf, own_rows, wb_o, 0, 2)
        co = scatter_begin(0)
        wide_stage(unit, obuf, own_rows, wb_o, 2, 4)
        with jax.named_scope('sum_o%d' % layer):
            scatter_next(0, co)
            if layer == 0:
                service(('g', 0))
            else:
                service(('u', layer))
                send_own(('d', layer))
            co[2].wait_recv()
            add(0, fin1, eighth, [r2.at[0]], fin.at[0])
            co[3].wait_recv()
            add(0, fin2, eighth, [r2.at[1]], fin.at[1])
        drain(co)
        with jax.named_scope('norm_o%d' % layer):
            add_norm(2 * layer, 3 * layer + 1)

    def mlp_stage(layer):
        cs = [spread_first(4, own_rows, 0), spread_first(4, own_rows, 1)]
        ex = []
        for k, start in ((16, fin1), (17, fin2)):
            ex.append(send(k, hid.at[own_rows, cols(start, eighth)], hid.at[pair_rows, cols(start, eighth)],
                           {'fsdp': pair}))
        if layer == 0:
            service(('u', 0))
            send_own(('d', 0))
        with jax.named_scope('spread_h%d' % layer):
            spread_next(4, own_rows, cs)
        with jax.named_scope('pair_h%d' % layer):
            ex[0].wait_recv()
            ch = [spread_first(12, pair_rows, 0)]
            ex[1].wait_recv()
            ch.append(spread_first(12, pair_rows, 1))
        finish(('g', layer))
        finish(('u', layer))
        gu_fetch(layer, 0, gu_tile, 0)
        with jax.named_scope('spread_h_last%d' % layer):
            cs[2].wait_recv()
            cs[3].wait_recv()

        def pair_next():
            ch[0].wait_recv()
            spread_copy(12, pair_rows, 2).start()
            ch[1].wait_recv()
            spread_copy(12, pair_rows, 3).start()
            if layer > 0:
                service(('d', layer))

        with jax.named_scope('gu_own%d' % layer):
            gu_tiles(layer, own_rows, gu_whole // 2, pair_next)
        gu_fetch(layer, 0, gu_tile, 0)
        with jax.named_scope('pair_h_last%d' % layer):
            for i in (2, 3):
                ch.append(spread_copy(12, pair_rows, i))
                ch[i].wait_recv()
        if layer == 0:
            service(('d', 0))
        if layer + 1 < n_layers:
            send_own(('o', layer + 1))
            send_own(('q', layer + 1))
        with jax.named_scope('gu_pair%d' % layer):
            gu_tiles(layer, pair_rows, 0, None)
        drain(ex + cs + ch)

        unit = ('d', layer)
        finish(unit)
        wide_fetch(unit, wb_d, 0, 0)
        all_rows = pl.ds(0, 2 * tokens)
        wide_stage(unit, act, all_rows, wb_d, 0, 2)
        cp = scatter_begin(1)
        wide_stage(unit, act, all_rows, wb_d, 2, 4)
        with jax.named_scope('sum_d_pair%d' % layer):
            scatter_next(1, cp)
            co = scatter_begin(0)
            cp[2].wait_recv()
            add(tokens, fin1, eighth, [r2.at[2]])
            ce = [send(18, part.at[pair_rows, cols(fin1, eighth)], pr.at[0], {'fsdp': pair})]
            cp[3].wait_recv()
            add(tokens, fin2, eighth, [r2.at[3]])
            ce.append(send(19, part.at[pair_rows, cols(fin2, eighth)], pr.at[1], {'fsdp': pair}))
        with jax.named_scope('sum_d_next%d' % layer):
            scatter_next(0, co)
        with jax.named_scope('sum_d_last%d' % layer):
            co[2].wait_recv()
            ce[0].wait_recv()
            add(0, fin1, eighth, [r2.at[0], pr.at[0]], fin.at[0])
            co[3].wait_recv()
            ce[1].wait_recv()
            add(0, fin2, eighth, [r2.at[1], pr.at[1]], fin.at[1])
        with jax.named_scope('norm_d%d' % layer):
            add_norm(2 * layer + 1, 3 * layer + 2)
        cs = [spread_first(4, own_rows, 0), spread_first(4, own_rows, 1)]
        if layer + 1 < n_layers:
            service(('o', layer + 1))
            service(('q', layer + 1))
            send_own(('g', layer + 1))
            send_own(('u', layer + 1))
        with jax.named_scope('sum_d_spread%d' % layer):
            spread_next(4, own_rows, cs)
            cs[2].wait_recv()
            cs[3].wait_recv()
        drain(cp + co + ce + cs)

    for d in range(1, n_f):
        rcopy(gains, gbuf.at[f], g_send, g_recv, {'fsdp': lax.rem(f + d, n_f)}).start()
    send_own(('q', 0))
    load_x = pltpu.make_async_copy(x_in, hid.at[own_rows], io_sem.at[2])
    load_x.start()
    gbuf[f] = gains[...]
    load_x.wait()
    wait_bytes(gbuf.at[pl.ds(0, n_f - 1)], g_recv)
    wait_bytes(gbuf.at[pl.ds(0, n_f - 1)], g_send)
    service(('q', 0))
    send_own(('o', 0))

    for layer in range(n_layers):
        qkv_stage(layer)
        ck, cv = attention_stage(layer)
        if layer > 0:
            service(('g', layer))
        finish(('o', layer))
        out_stage(layer)
        ck.wait()
        cv.wait()
        mlp_stage(layer)

    store_y = pltpu.make_async_copy(hid.at[own_rows], y_out, io_sem.at[2])
    store_y.start()
    for u in range(n_units):
        wait_bytes(units[order[u]][0].at[pl.ds(0, 7)], unit_send.at[u])
    store_y.wait()


def solution(mesh):
    batch_axes = ('dp', 'fsdp')
    act_spec = P(batch_axes, None, None)
    in_cols = P(None, 'fsdp', 'tp')
    in_rows = P(None, 'tp', 'fsdp')
    tp_gain = P(None, 'tp')
    fsdp_gain = P(None, 'fsdp')
    cache_spec = P(None, batch_axes, None, 'tp', None)
    n_f, n_t = mesh.shape['fsdp'], mesh.shape['tp']

    def local_layers(x, w_query, w_key, w_value, w_out, w_gate, w_up, w_down, q_norm_w, k_norm_w, attn_norm_w, ffn_norm_w):
        batch, seq_len, width = x.shape
        n_layers, shard, hw = w_query.shape
        ff = w_gate.shape[2]
        tokens = batch * seq_len
        gains = jnp.stack([attn_norm_w, ffn_norm_w], axis=1).reshape(2 * n_layers, shard)
        gain_rows = -(-2 * n_layers // 8) * 8
        gains = jnp.pad(gains, ((0, gain_rows - 2 * n_layers), (0, 0)))
        cos_t, sin_t = rope_tables(seq_len)
        hbm = pl.BlockSpec(memory_space=pl.ANY)
        vmem = pl.BlockSpec(memory_space=pltpu.VMEM)
        w_gate, w_up = w_gate.transpose(0, 2, 1), w_up.transpose(0, 2, 1)
        ff_half = ff // 2
        layer_bufs = [jax.ShapeDtypeStruct((n_f, 3, shard, hw), BF16), jax.ShapeDtypeStruct((n_f, 1, hw, shard), BF16),
                      jax.ShapeDtypeStruct((n_f, 1, ff_half, shard), BF16),
                      jax.ShapeDtypeStruct((n_f, 1, ff_half, shard), BF16),
                      jax.ShapeDtypeStruct((n_f, 1, ff_half, shard), BF16)]
        out_shape = [jax.ShapeDtypeStruct((tokens, width), BF16), jax.ShapeDtypeStruct((n_layers, tokens, hw), BF16),
                     jax.ShapeDtypeStruct((n_layers, tokens, hw), BF16)] + layer_bufs * n_layers
        sq_rows = -(-2 * (tokens // 128) // 8) * 8
        scratch = [
            pltpu.VMEM((2 * tokens, width), BF16),
            pltpu.VMEM((3, tokens, hw), F32),
            pltpu.VMEM((tokens, hw), BF16),
            pltpu.VMEM((tokens, hw), BF16),
            pltpu.VMEM((tokens, hw), BF16),
            pltpu.VMEM((2 * tokens, ff_half), BF16),
            pltpu.VMEM((2 * tokens, width), BF16),
            pltpu.VMEM((2, tokens, width // 8), BF16),
            pltpu.VMEM((4, tokens, width // 4), BF16),
            pltpu.VMEM((4, tokens, width // 8), BF16),
            pltpu.VMEM((2, tokens, width // 8), BF16),
            pltpu.VMEM((3 * n_layers, n_t, sq_rows, 128), F32),
            pltpu.VMEM((tokens, 128), F32),
            pltpu.VMEM((n_f, gain_rows, shard), F32),
            pltpu.VMEM((2, 6 * shard, min(256, hw)), BF16),
            pltpu.VMEM((2, 2, min(256, ff_half), width), BF16),
            pltpu.VMEM((2, 2, hw, shard), BF16),
            pltpu.VMEM((2, 2, ff_half, shard), BF16),
            pltpu.SemaphoreType.DMA((5 * n_layers, 8)),
            pltpu.SemaphoreType.DMA((5 * n_layers,)),
            pltpu.SemaphoreType.DMA((2,)),
            pltpu.SemaphoreType.DMA((20,)),
            pltpu.SemaphoreType.DMA((20,)),
            pltpu.SemaphoreType.DMA((3 * n_layers, n_t - 1)),
            pltpu.SemaphoreType.DMA((3 * n_layers, n_t - 1)),
            pltpu.SemaphoreType.DMA,
            pltpu.SemaphoreType.DMA,
            pltpu.SemaphoreType.DMA((3,)),
        ]
        outs = pl.pallas_call(
            lambda *refs: layers_kernel(n_f, n_t, n_layers, *refs),
            name='layers',
            out_shape=out_shape,
            in_specs=[hbm] * 8 + [vmem] * 5,
            out_specs=[hbm] * len(out_shape),
            scratch_shapes=scratch,
            compiler_params=pltpu.CompilerParams(collective_id=0, has_side_effects=True, vmem_limit_bytes=66 * 1000 * 1000),
        )(x.reshape(tokens, width), w_query, w_key, w_value, w_out, w_gate, w_up, w_down,
          q_norm_w, k_norm_w, gains, cos_t, sin_t)
        cache_shape = (n_layers, batch, seq_len, hw // HEAD_DIM, HEAD_DIM)
        return outs[0].reshape(batch, seq_len, width), outs[1].reshape(cache_shape), outs[2].reshape(cache_shape)

    return jax.shard_map(local_layers, mesh=mesh,
                         in_specs=(act_spec, in_cols, in_cols, in_cols, in_rows, in_cols, in_cols, in_rows,
                                   tp_gain, tp_gain, fsdp_gain, fsdp_gain),
                         out_specs=(act_spec, cache_spec, cache_spec), check_vma=False)
```
